128 devices in a mesh: seq: 32 (over x, z, core), head: 4 (over y).
Axes of the slice: x: 4, y: 4, z: 4, core: 2. Of those that a mesh axis runs over, the one named last changes fastest.
Arguments:
- queries: bfloat16 [24576, 8192], P('seq', 'head'), may hold values from -6 to 6
- key_rows: bfloat16 [24576, 8192], P('seq', 'head'), may hold values from -0.5 to 0.5
- value_rows: bfloat16 [24576, 8192], P('seq', 'head'), may hold values from -130 to 130
- log_decay: float32 [64, 24576], P('head', 'seq'), may hold values from -1 to 0
- norm_gain: float32 [8192], P('head'), may hold values from 0.1 to 1.9
- grad_out: bfloat16 [24576, 8192], P('seq', 'head'), may hold values from -13 to 13
Outputs:
- output: bfloat16 [24576, 8192], P('seq', 'head')
- grad_queries: bfloat16 [24576, 8192], P('seq', 'head')
- grad_keys: bfloat16 [24576, 8192], P('seq', 'head')
- grad_values: bfloat16 [24576, 8192], P('seq', 'head')
- grad_gain: float32 [8192], P('head')
The draws below stay inside these ranges and needn't reach their ends.
All inputs are finite; a program needn't handle non-finite values.
Results may differ from the reference program's by a relative error of at most 0.01.
Values sent between devices are 32-bit elements; how exact they have to be, the bound alone decides.
A program may use at most 192 MiB of HBM per device.

```python
import jax
import jax.numpy as jnp
from jax import lax

HEADS = 64
DH = 128
TOK_DEV = 768
SEQUENCE_TOKENS = 24576
HD = 8192


def draw_log_decay(key, part):
    sample_sequences = jax.random.split(key, 6)
    token_position = jnp.arange(SEQUENCE_TOKENS)
    fast_share = 0.5
    picked = jax.random.uniform(sample_sequences[0], (HEADS, 1), dtype=jnp.float32)
    fast_rate = jnp.exp(jax.random.uniform(sample_sequences[1], (HEADS, 1), dtype=jnp.float32, minval=jnp.log(1.0 / 50.0), maxval=jnp.log(1.0 / 30.0)))
    slow_rate = 0.6 / SEQUENCE_TOKENS
    baseline_decay_rate = jnp.where(picked < fast_share, fast_rate, slow_rate)
    block_count = SEQUENCE_TOKENS // TOK_DEV
    block_multiplier = jnp.exp(jax.random.uniform(sample_sequences[2], (HEADS, block_count), dtype=jnp.float32, minval=jnp.log(0.5), maxval=jnp.log(2.0)))
    block_multiplier = jnp.repeat(block_multiplier, TOK_DEV, axis=1, total_repeat_length=SEQUENCE_TOKENS)
    jitter_amplitude = jax.random.uniform(sample_sequences[3], (HEADS, SEQUENCE_TOKENS), dtype=jnp.float32, minval=0.5, maxval=1.5)
    spike_locations = jax.random.randint(sample_sequences[4], (3,), 0, SEQUENCE_TOKENS)
    spike_magnitude = jax.random.uniform(sample_sequences[5], (HEADS, 3), dtype=jnp.float32, minval=0.22, maxval=0.69)
    decay_spikes = jnp.sum(jnp.where(token_position[None, :, None] == spike_locations[None, None, :], spike_magnitude[:, None, :], 0.0), axis=2)
    return (-(baseline_decay_rate * block_multiplier * jitter_amplitude + decay_spikes)).astype(jnp.float32)


def draw_value_rows(key, part):
    sample_sequences = jax.random.split(key, 3)
    head_number = (jnp.arange(HD) // DH).astype(jnp.float32)
    head_scale = 1.0 + 2.0 * head_number / max(HEADS - 1, 1)
    base = jnp.clip(jax.random.normal(sample_sequences[0], (SEQUENCE_TOKENS, HD), dtype=jnp.float32), -4.0, 4.0)
    row_scale = jnp.exp(jax.random.uniform(sample_sequences[2], (SEQUENCE_TOKENS, 1), dtype=jnp.float32, minval=0.0, maxval=jnp.log(10.0)))
    return (base * head_scale[None, :] * row_scale).astype(jnp.bfloat16)


def draw_grad_out(key, part):
    sample_sequences = jax.random.split(key, 1)
    ramp = 1.0 + 2.0 * jnp.arange(SEQUENCE_TOKENS).astype(jnp.float32) / (SEQUENCE_TOKENS - 1)
    base = jnp.clip(jax.random.normal(sample_sequences[0], (SEQUENCE_TOKENS, HD), dtype=jnp.float32), -4.0, 4.0)
    return (base * ramp[:, None]).astype(jnp.bfloat16)


def level_of(rng, dims, cuts, least, largest):
    def one(axis_at, parts):
        draws = jax.random.uniform(jax.random.fold_in(jax.random.fold_in(rng, 6), axis_at), (parts,), jnp.float32, least / len(cuts), largest / len(cuts))
        return jnp.repeat(jnp.exp(draws), dims[axis_at] // parts).reshape((-1,) + (1,) * (len(dims) - axis_at - 1))

    factor_of = one(*cuts[0])
    for cut in cuts[1:]:
        factor_of = factor_of * one(*cut)
    return factor_of


def normal_values(rng, extent, width, limit, cuts=(), held_as=jnp.bfloat16):
    result = jax.random.normal(rng, extent, jnp.float32) * width
    if len(cuts) > 0:
        result = level_of(rng, extent, cuts, -0.22, 0.18) * result
    return jnp.clip(result, min=-limit, max=limit).astype(held_as)


def setup_inputs(seed: int = 0) -> dict:
    arg_keys = jax.random.split(jax.random.key(seed), 7)
    queries = normal_values(arg_keys[0], (SEQUENCE_TOKENS, HD), 1.0, 6.0, ((0, 32), (1, 4)))
    key_rows = normal_values(arg_keys[1], (SEQUENCE_TOKENS, HD), DH ** -0.5, 0.5, ((0, 32), (1, 4)))
    value_rows = draw_value_rows(jax.random.fold_in(arg_keys[6], 71), 0)
    log_decay = draw_log_decay(jax.random.fold_in(arg_keys[6], 71), 0)
    norm_gain = jnp.clip(1.0 + 0.18 * jax.random.normal(arg_keys[4], (HD,), jnp.float32), 0.1, 1.9)
    grad_out = draw_grad_out(jax.random.fold_in(arg_keys[6], 71), 0)
    return dict(queries=queries, key_rows=key_rows, value_rows=value_rows, log_decay=log_decay, norm_gain=norm_gain, grad_out=grad_out)


EPSILON = 1e-06

def exact_product(form, left, right):
    return jnp.einsum(form, left.astype(jnp.float32), right.astype(jnp.float32), precision=lax.Precision.HIGHEST)

def plain_product(form, left, right):
    return jnp.einsum(form, left.astype(jnp.float32), right.astype(jnp.float32))

def causal_decay(cumulative):
    length = cumulative.shape[-1]
    below_diag = jnp.arange(length)[:, None] >= jnp.arange(length)[None, :]
    spread = cumulative[..., :, None] - cumulative[..., None, :]
    return jnp.where(below_diag, jnp.exp(jnp.where(below_diag, spread, 0.0)), 0.0)

def split_heads(matrix):
    return matrix.reshape(matrix.shape[0], HEADS, DH).transpose(1, 0, 2)

def merge_heads(tensor):
    return tensor.transpose(1, 0, 2).reshape(tensor.shape[1], HD)

def attend(q_heads, k_heads, v_heads, cumulative, state):
    decay_mask = causal_decay(cumulative)
    scores = plain_product('htd,hsd->hts', q_heads, k_heads)
    weights = (scores * decay_mask).astype(jnp.bfloat16)
    attended = plain_product('hts,hsd->htd', weights, v_heads)
    attended = attended + jnp.exp(cumulative)[..., None] * exact_product('htd,hde->hte', q_heads, state)
    return (attended, weights, decay_mask)

def normalize(attended, grad_rows, norm_gain):
    mixed = merge_heads(attended)
    inverse = lax.rsqrt(lax.optimization_barrier(jnp.mean(mixed * mixed, axis=1)) + EPSILON)
    normed = mixed * inverse[:, None]
    scaled = grad_rows.astype(jnp.float32) * norm_gain[None, :]
    center = lax.optimization_barrier(jnp.mean(scaled * normed, axis=1))
    grad_attended = (inverse[:, None] * (scaled - normed * center[:, None])).astype(jnp.bfloat16)
    return (normed, split_heads(grad_attended))

def reference(queries, key_rows, value_rows, log_decay, norm_gain, grad_out):
    blocks = SEQUENCE_TOKENS // TOK_DEV

    def tile(matrix):
        return matrix.reshape(blocks, TOK_DEV, HEADS, DH).transpose(0, 2, 1, 3)
    q_all = tile(queries)
    k_all = tile(key_rows)
    v_all = tile(value_rows)
    grad_rows = grad_out.reshape(blocks, TOK_DEV, HD)
    cumulative = jnp.cumsum(log_decay.reshape(HEADS, blocks, TOK_DEV).transpose(1, 0, 2), axis=2)
    block_total = cumulative[:, :, -1]

    def local_fn(operands):
        k_heads, v_heads, cumul, last_value = operands
        tail = jnp.exp(last_value[:, None] - cumul)
        return exact_product('htd,hte->hde', k_heads.astype(jnp.float32) * tail[..., None], v_heads)
    local_state = lax.map(local_fn, (k_all, v_all, cumulative, block_total))

    def carry_step(carry, operands):
        decay_total, local_term = operands
        return (decay_total[:, None, None] * carry + local_term, carry)
    zero_state = jnp.zeros((HEADS, DH, DH), jnp.float32)
    _, state_in = lax.scan(carry_step, zero_state, (jnp.exp(block_total), local_state))

    def second_pass(operands):
        q_heads, k_heads, v_heads, grad_block, cumul, state = operands
        attended, _, _ = attend(q_heads, k_heads, v_heads, cumul, state)
        normed, grad_heads = normalize(attended, grad_block, norm_gain)
        output_block = (normed * norm_gain[None, :]).astype(jnp.bfloat16)
        gain_part = lax.optimization_barrier(jnp.sum(grad_block.astype(jnp.float32) * normed, axis=0))
        state_grad = exact_product('htd,hte->hde', q_heads.astype(jnp.float32) * jnp.exp(cumul)[..., None], grad_heads)
        return (output_block, gain_part, state_grad)
    output, gain_parts, state_grad = lax.map(second_pass, (q_all, k_all, v_all, grad_rows, cumulative, state_in))
    _, state_after = lax.scan(carry_step, zero_state, (jnp.exp(block_total), state_grad), reverse=True)

    def fourth_pass(operands):
        q_heads, k_heads, v_heads, grad_block, cumul, last_value, state, after = operands
        attended, weights, decay_mask = attend(q_heads, k_heads, v_heads, cumul, state)
        _, grad_heads = normalize(attended, grad_block, norm_gain)
        grad_weights = (plain_product('htd,hsd->hts', grad_heads, v_heads) * decay_mask).astype(jnp.bfloat16)
        tail = jnp.exp(last_value[:, None] - cumul)[..., None]
        grad_q = plain_product('hts,hsd->htd', grad_weights, k_heads)
        grad_q = grad_q + jnp.exp(cumul)[..., None] * exact_product('hte,hde->htd', grad_heads, state)
        grad_k = plain_product('hts,htd->hsd', grad_weights, q_heads)
        grad_k = grad_k + tail * exact_product('hse,hde->hsd', v_heads, after)
        grad_v = plain_product('hts,htd->hsd', weights, grad_heads)
        grad_v = grad_v + tail * exact_product('hsd,hde->hse', k_heads, after)
        return (merge_heads(grad_q).astype(jnp.bfloat16), merge_heads(grad_k).astype(jnp.bfloat16), merge_heads(grad_v).astype(jnp.bfloat16))
    grad_q, grad_k, grad_v = lax.map(fourth_pass, (q_all, k_all, v_all, grad_rows, cumulative, block_total, state_in, state_after))
    grad_gain = lax.optimization_barrier(jnp.sum(gain_parts, axis=0))
    return (output.reshape(SEQUENCE_TOKENS, HD), grad_q.reshape(SEQUENCE_TOKENS, HD), grad_k.reshape(SEQUENCE_TOKENS, HD), grad_v.reshape(SEQUENCE_TOKENS, HD), grad_gain)
```

```python
import functools

import jax
import jax.numpy as jnp
from jax import lax
from jax.experimental import pallas as pl
from jax.experimental.pallas import tpu as pltpu
from jax.sharding import PartitionSpec as P

DH = 128
EPSILON = 1e-06
CHUNK = 256
SPLIT_FORWARD = 8
SPLIT_BACKWARD = 8
F32 = jnp.float32
BF16 = jnp.bfloat16
MESH = pl.DeviceIdType.MESH
HIGHEST = lax.Precision.HIGHEST


def mm(left, right, dims):
    return lax.dot_general(left, right, (dims, ((), ())), preferred_element_type=F32)


AB = ((1,), (0,))
ABT = ((1,), (1,))
ATB = ((0,), (0,))


def chunk_cumsum(ld_ref, cum_ref, chunk):
    below = lax.broadcasted_iota(jnp.int32, (chunk, chunk), 0)
    right = lax.broadcasted_iota(jnp.int32, (chunk, chunk), 1)
    tri = (below <= right).astype(F32)
    for j in range(ld_ref.shape[1] // chunk):
        span = slice(j * chunk, (j + 1) * chunk)
        cum_ref[:, span] = lax.dot_general(
            ld_ref[:, span], tri, (AB, ((), ())), precision=HIGHEST, preferred_element_type=F32
        )


def cum_forms(cum_ref, h, j, chunk):
    row = cum_ref[pl.ds(h, 1), j * chunk : (j + 1) * chunk]
    column = jnp.broadcast_to(row, (DH, chunk)).T
    return row, column


def decay_of(row, column):
    chunk = row.shape[1]
    wide = jnp.concatenate([column] * (chunk // DH), axis=1)
    t = lax.broadcasted_iota(jnp.int32, (chunk, chunk), 0)
    s = lax.broadcasted_iota(jnp.int32, (chunk, chunk), 1)
    return jnp.where(t >= s, jnp.exp(wide - row), 0.0)


def remote(src, dst, send, recv, axis, target):
    return pltpu.make_async_remote_copy(
        src_ref=src, dst_ref=dst, send_sem=send, recv_sem=recv,
        device_id={axis: target}, device_id_type=MESH,
    )


def loop(count, body):
    lax.fori_loop(0, count, lambda i, c: (body(i), c)[1], 0)


class Scan:
    def __init__(self, n, reverse, bufs, decays=None):
        (
            self.lsend, self.lrecv, self.own, self.csend, self.arecv, self.asend, self.brecv,
            self.xsend, self.xrecv, self.lsem, self.asend_sem, self.arecv_sem,
            self.bsend_sem, self.brecv_sem, self.xsem,
        ) = bufs
        self.reverse = reverse
        self.chips = n // 2
        self.led = self.lsend.shape[0]
        self.half = self.led * DH // self.chips
        self.parts = DH // self.half
        me = lax.axis_index("seq")
        self.core = lax.rem(me, 2)
        self.chip = me // 2
        self.partner = me + 1 - 2 * self.core
        self.am_first = self.core == (1 if reverse else 0)
        self.mine = self.chip // self.parts
        self.part = lax.rem(self.chip, self.parts)
        self.back = self.half + 8 if reverse else self.half
        self.cross = DH + 8 if reverse else DH
        self.decays = self if decays is None else decays

    def copy_l(self, j):
        return remote(self.lsend.at[j], self.lrecv.at[j], self.lsem.at[0, j], self.lsem.at[1, j], "seq", self.partner)

    def copy_a(self, j, b, chip):
        return remote(
            self.csend.at[j, b], self.arecv.at[chip], self.asend_sem.at[j, b], self.arecv_sem.at[chip],
            "seq", 2 * (self.parts * j + b) + self.core,
        )

    def copy_b(self, c, j, b):
        rows = pl.ds(0, self.back)
        return remote(
            self.asend.at[c, rows], self.brecv.at[j, b, rows], self.bsend_sem.at[c], self.brecv_sem.at[j, b],
            "seq", 2 * c + self.core,
        )

    def copy_x(self, j):
        rows = pl.ds(0, self.cross)
        return remote(self.xsend.at[j, rows], self.xrecv.at[j, rows], self.xsem.at[0, j], self.xsem.at[1, j], "seq", self.partner)

    def away(self, j, b):
        return self.parts * j + b != self.chip

    def give(self, j, state, extra):
        self.lsend[j, 0:DH] = state
        self.lsend[j, DH : DH + 8] = jnp.broadcast_to(extra, (8, DH))

    def keep(self, j, state, extra):
        self.own[j, 0:DH] = state
        self.own[j, DH : DH + 8] = jnp.broadcast_to(extra, (8, DH))
        self.copy_l(j).wait_recv()
        theirs = self.lrecv[j, 0:DH]
        first = jnp.where(self.am_first, state, theirs)
        second = jnp.where(self.am_first, theirs, state)
        mine, other = self.decays.own[j, DH : DH + 8], self.decays.lrecv[j, DH : DH + 8]
        decay_second = jnp.where(self.am_first, other, mine)[0:1]
        both = decay_second * first + second
        tail = self.own[j, DH : DH + 8] + self.lrecv[j, DH : DH + 8] if self.reverse else mine * other
        for b in range(self.parts):
            self.csend[j, b, 0 : self.half] = both[b * self.half : (b + 1) * self.half]
            self.csend[j, b, self.half : self.half + 8] = tail

            @pl.when(self.away(j, b))
            def _():
                self.copy_a(j, b, self.chip).start()

            @pl.when(jnp.logical_not(self.away(j, b)))
            def _():
                self.arecv[self.chip] = self.csend[j, b]

    def combine(self):
        def arrive(c):
            @pl.when(c != self.chip)
            def _():
                self.copy_a(self.mine, self.part, c).wait_recv()

        if self.reverse:
            loop(self.chips, arrive)
            total = self.arecv[0, self.half : self.half + 8]
            for c in range(1, self.chips):
                total = total + self.arecv[c, self.half : self.half + 8]

        def one(i, state):
            c = self.chips - 1 - i if self.reverse else i
            if not self.reverse:
                arrive(c)
            self.asend[c, 0 : self.half] = state
            if self.reverse:
                self.asend[c, self.half : self.half + 8] = total

            @pl.when(c != self.chip)
            def _():
                self.copy_b(c, self.mine, self.part).start()

            @pl.when(c == self.chip)
            def _():
                self.brecv[self.mine, self.part, 0 : self.back] = self.asend[c, 0 : self.back]

            decay = self.decays.arecv[c, self.half : self.half + 1]
            return decay * state + self.arecv[c, 0 : self.half]

        lax.fori_loop(0, self.chips, one, jnp.zeros((self.half, DH), F32))

    def take(self, j, state_in):
        for b in range(self.parts):
            @pl.when(self.away(j, b))
            def _():
                self.copy_b(self.chip, j, b).wait_recv()

        base = jnp.concatenate([self.brecv[j, b, 0 : self.half] for b in range(self.parts)], axis=0)
        decay = jnp.where(self.am_first, self.decays.own[j, DH : DH + 8], self.decays.lrecv[j, DH : DH + 8])[0:1]
        held = jnp.where(self.am_first, self.own[j, 0:DH], self.lrecv[j, 0:DH])
        after = decay * base + held
        state_in[j] = jnp.where(self.am_first, base, after)
        self.xsend[j, 0:DH] = jnp.where(self.am_first, after, base)
        if self.reverse:
            self.xsend[j, DH : DH + 8] = self.brecv[j, 0, self.half : self.half + 8]
        self.copy_x(j).start()

    def finish(self, j):
        self.copy_l(j).wait_send()
        self.copy_x(j).wait_send()
        for b in range(self.parts):
            @pl.when(self.away(j, b))
            def _():
                self.copy_a(j, b, self.chip).wait_send()

    def finish_chip(self, c):
        @pl.when(c != self.chip)
        def _():
            self.copy_b(c, self.mine, self.part).wait_send()


def main_kernel(
    n, peers, chunk,
    q_hbm, k_hbm, v_hbm, g_hbm, ld_ref, gain_ref,
    q, k, v, g, att, obuf, r_out, cum_ref, gg_out,
    s_out, lc, state_in, sq_acc, in_acc,
    stat_send, stat_recv, inv_b, cen_b, *rest,
):
    load_sem, stat_sem = rest[-2:]
    bufs1, bufs2 = rest[:15], rest[15:30]
    heads, tokens, _ = q.shape
    chunks = tokens // chunk
    me = lax.axis_index("seq")
    my_head = lax.axis_index("head")
    columns = heads * DH * peers

    def load(i, hbm, vmem, h):
        where = pl.ds(pl.multiple_of(h * DH, DH), DH)
        return pltpu.make_async_copy(hbm.at[:, where], vmem.at[h], load_sem.at[i, h])

    def load_kv(h):
        load(0, k_hbm, k, h).start()
        load(1, v_hbm, v, h).start()

    def load_q(h):
        load(2, q_hbm, q, h).start()

    def load_g(h):
        load(3, g_hbm, g, h).start()

    barrier = pltpu.get_barrier_semaphore()
    for off in range(1, n // 2):
        pl.semaphore_signal(barrier, inc=1, device_id={"seq": lax.rem(me + 2 * off, n)}, device_id_type=MESH)
    pl.semaphore_signal(barrier, inc=1, device_id={"seq": me + 1 - 2 * lax.rem(me, 2)}, device_id_type=MESH)
    for off in range(1, peers):
        pl.semaphore_signal(barrier, inc=1, device_id={"head": lax.rem(my_head + off, peers)}, device_id_type=MESH)


    forward = Scan(n, False, bufs1)
    backward = Scan(n, True, bufs2, forward)
    core, led = forward.core, forward.led

    def led_head(j):
        return 2 * j + core

    def other_head(j):
        return 2 * j + 1 - core

    def turned(i):
        return lax.rem(i + forward.mine + 1, led)

    loop(led, lambda j: load_kv(other_head(j)))
    loop(led, lambda i: load_kv(led_head(turned(i))))
    loop(heads, load_q)
    loop(heads, load_g)
    chunk_cumsum(ld_ref, cum_ref, chunk)

    def local_state(h):
        load(0, k_hbm, k, h).wait()
        load(1, v_hbm, v, h).wait()
        state = None
        for j in range(chunks):
            span = slice(j * chunk, (j + 1) * chunk)
            _, column = cum_forms(cum_ref, h, j, chunk)
            total = column[chunk - 1 : chunk, :]
            tail = jnp.exp(total - column)
            part = mm((k[h, span].astype(F32) * tail).astype(BF16), v[h, span], ATB)
            lc[h, j] = part
            state = part if j == 0 else jnp.exp(total) * state + part
            decay = total if j == 0 else decay + total
        return state, jnp.exp(decay)

    def give_forward(j):
        forward.give(j, *local_state(other_head(j)))

    def keep_forward(i):
        j = turned(i)
        forward.keep(j, *local_state(led_head(j)))

    loop(led, give_forward)
    pl.semaphore_wait(barrier, n // 2 - 1 + 1 + peers - 1)
    loop(led, lambda j: forward.copy_l(j).start())
    loop(led, keep_forward)

    def intra(h):
        load(2, q_hbm, q, h).wait()
        for j in range(chunks):
            span = slice(j * chunk, (j + 1) * chunk)
            row, column = cum_forms(cum_ref, h, j, chunk)
            scores = mm(q[h, span], k[h, span], ABT)
            weights = (scores * decay_of(row, column)).astype(BF16)
            att[h, span] = mm(weights, v[h, span], AB)

    loop(SPLIT_FORWARD, intra)
    forward.combine()
    loop(heads - SPLIT_FORWARD, lambda i: intra(i + SPLIT_FORWARD))
    loop(led, lambda j: forward.take(j, state_in))

    sq_acc[...] = jnp.zeros_like(sq_acc)
    in_acc[...] = jnp.zeros_like(in_acc)

    def inter(h, state):
        load(3, g_hbm, g, h).wait()
        gain = gain_ref[pl.ds(h, 1), :]
        for j in range(chunks):
            span = slice(j * chunk, (j + 1) * chunk)
            _, column = cum_forms(cum_ref, h, j, chunk)
            rounded = state.astype(BF16)
            s_out[h, j] = rounded
            whole = att[h, span] + jnp.exp(column) * mm(q[h, span], rounded, AB)
            att[h, span] = whole
            sq_acc[span] += whole * whole
            in_acc[span] += g[h, span].astype(F32) * gain * whole
            if j < chunks - 1:
                state = jnp.exp(column[chunk - 1 : chunk, :]) * state + lc[h, j]

    def inter_other(j):
        forward.copy_x(j).wait_recv()
        inter(other_head(j), forward.xrecv[j, 0:DH])

    loop(led, lambda j: inter(led_head(j), state_in[j]))
    loop(led, inter_other)

    ones = jnp.ones((8, DH), F32)

    def row_sums(acc):
        return lax.dot_general(ones, acc, (ABT, ((), ())), precision=HIGHEST, preferred_element_type=F32)

    upper = lax.broadcasted_iota(jnp.int32, (8, tokens), 0) < 4
    stat_send[...] = jnp.where(upper, row_sums(sq_acc[...]), row_sums(in_acc[...]))

    def stat_copy(off, slot):
        return remote(stat_send, stat_recv.at[slot], stat_sem.at[0, off], stat_sem.at[1, off], "head", lax.rem(my_head + off, peers))

    for off in range(1, peers):
        stat_copy(off, my_head).start()
    stat_recv[my_head] = stat_send[...]
    for off in range(1, peers):
        stat_copy(off, lax.rem(my_head + peers - off, peers)).wait_recv()
    stats = stat_recv[0]
    for i in range(1, peers):
        stats = stats + stat_recv[i]
    inverse = lax.rsqrt(stats[0:1] / columns + EPSILON)
    center = stats[4:5] * inverse / columns
    inv_b[...] = jnp.broadcast_to(inverse, (DH, tokens)).T
    cen_b[...] = jnp.broadcast_to(center, (DH, tokens)).T

    def normalize(h):
        gain = gain_ref[pl.ds(h, 1), :]
        gain_part = jnp.zeros((1, DH), F32)
        state = None
        for j in reversed(range(chunks)):
            span = slice(j * chunk, (j + 1) * chunk)
            _, column = cum_forms(cum_ref, h, j, chunk)
            normed = att[h, span] * inv_b[span]
            obuf[h, span] = (normed * gain).astype(BF16)
            cotangent = g[h, span].astype(F32)
            gain_part = gain_part + jnp.sum(cotangent * normed, axis=0, keepdims=True)
            grad = (inv_b[span] * (cotangent * gain - normed * cen_b[span])).astype(BF16)
            g[h, span] = grad
            part = mm((q[h, span].astype(F32) * jnp.exp(column)).astype(BF16), grad, ATB)
            lc[h, j] = part
            total = column[chunk - 1 : chunk, :]
            state = part if state is None else jnp.exp(total) * state + part
        return state, gain_part

    def give_backward(j):
        backward.give(j, *normalize(other_head(j)))
        backward.copy_l(j).start()

    def keep_backward(i):
        j = turned(i)
        backward.keep(j, *normalize(led_head(j)))

    loop(led, give_backward)
    loop(led, keep_backward)

    def gradients(h):
        for j in range(chunks):
            span = slice(j * chunk, (j + 1) * chunk)
            row, column = cum_forms(cum_ref, h, j, chunk)
            decay = decay_of(row, column)
            queries, keys, values, grad = q[h, span], k[h, span], v[h, span], g[h, span]
            weights = (mm(queries, keys, ABT) * decay).astype(BF16)
            grad_weights = (mm(grad, values, ABT) * decay).astype(BF16)
            q[h, span] = (
                mm(grad_weights, keys, AB) + jnp.exp(column) * mm(grad, s_out[h, j], ABT)
            ).astype(BF16)
            att[h, span] = mm(grad_weights, queries, ATB)
            g[h, span] = mm(weights, grad, ATB).astype(BF16)

    loop(SPLIT_BACKWARD, gradients)
    backward.combine()
    loop(heads - SPLIT_BACKWARD, lambda i: gradients(i + SPLIT_BACKWARD))
    loop(led, lambda j: backward.take(j, state_in))

    def after(h, state, gain_total):
        for j in reversed(range(chunks)):
            r_out[h, j] = state.astype(BF16)
            if j > 0:
                _, column = cum_forms(cum_ref, h, j, chunk)
                state = jnp.exp(column[chunk - 1 : chunk, :]) * state + lc[h, j]
        gg_out[pl.ds(h, 1), :] = gain_total

    def after_other(j):
        backward.copy_x(j).wait_recv()
        after(other_head(j), backward.xrecv[j, 0:DH], backward.xrecv[j, DH : DH + 1])

    loop(led, lambda j: after(led_head(j), state_in[j], backward.xsend[j, DH : DH + 1]))
    loop(led, after_other)

    def finish(j):
        forward.finish(j)
        backward.finish(j)

    def finish_chip(c):
        forward.finish_chip(c)
        backward.finish_chip(c)

    loop(led, finish)
    loop(n // 2, finish_chip)
    for off in range(1, peers):
        stat_copy(off, my_head).wait_send()


def last_kernel(
    chunk, k, v, gq, gk, gv, out, after, cum_ref,
    out_hbm, gq_hbm, gk_hbm, gv_hbm, k_stage, v_stage, store_sem,
):
    heads, tokens, _ = k.shape

    def store(i, vmem, hbm, h):
        where = pl.ds(pl.multiple_of(h * DH, DH), DH)
        return pltpu.make_async_copy(vmem.at[h], hbm.at[:, where], store_sem.at[i, h])

    def copies(h):
        return (
            store(0, out, out_hbm, h), store(1, gq, gq_hbm, h),
            store(2, k_stage, gk_hbm, h), store(3, v_stage, gv_hbm, h),
        )

    def one(h):
        ready = copies(h)
        ready[0].start()
        ready[1].start()
        for j in range(tokens // chunk):
            span = slice(j * chunk, (j + 1) * chunk)
            _, column = cum_forms(cum_ref, h, j, chunk)
            tail = jnp.exp(column[chunk - 1 : chunk, :] - column)
            k_stage[h, span] = (gk[h, span] + tail * mm(v[h, span], after[h, j], ABT)).astype(BF16)
            v_stage[h, span] = (
                gv[h, span].astype(F32) + tail * mm(k[h, span], after[h, j], AB)
            ).astype(BF16)
        ready[2].start()
        ready[3].start()

    def wait(h):
        for copy in copies(h):
            copy.wait()

    loop(heads, one)
    loop(heads, wait)


def on_device(n, peers, queries, key_rows, value_rows, log_decay, norm_gain, grad_out):
    tokens, width = queries.shape
    heads = width // DH
    chunk = CHUNK if tokens % CHUNK == 0 else tokens
    chunks = tokens // chunk
    gain = norm_gain.reshape(heads, DH)
    anywhere = pl.BlockSpec(memory_space=pl.ANY)
    vmem = pl.BlockSpec(memory_space=pltpu.VMEM)
    rows = jax.ShapeDtypeStruct((tokens, width), BF16)
    states = jax.ShapeDtypeStruct((heads, chunks, DH, DH), BF16)
    per_head = lambda *shape, dtype=F32: pltpu.VMEM((heads, *shape), dtype)
    dma = pltpu.SemaphoreType.DMA
    led, chips = heads // 2, n // 2
    half = led * DH // chips
    parts = DH // half
    buf = lambda *shape: pltpu.VMEM((*shape, DH), F32)
    scan = [
        buf(led, DH + 8), buf(led, DH + 8), buf(led, DH + 8), buf(led, parts, half + 8),
        buf(chips, half + 8), buf(chips, half + 8), buf(led, parts, half + 8),
        buf(led, DH + 8), buf(led, DH + 8),
        dma((2, led)), dma((led, parts)), dma((chips,)), dma((chips,)), dma((led, parts)), dma((2, led)),
    ]
    by_head = lambda dtype: pltpu.VMEM((heads, tokens, DH), dtype)
    *held, grad_gain = pl.pallas_call(
        functools.partial(main_kernel, n, peers, chunk),
        out_shape=(
            by_head(BF16), by_head(BF16), by_head(BF16), by_head(BF16), by_head(F32), by_head(BF16),
            pltpu.VMEM((heads, chunks, DH, DH), BF16), pltpu.VMEM((heads, tokens), F32),
            jax.ShapeDtypeStruct((heads, DH), F32),
        ),
        in_specs=[anywhere] * 4 + [vmem] * 2,
        out_specs=(vmem,) * 9,
        scratch_shapes=[
            per_head(chunks, DH, DH, dtype=BF16), per_head(chunks, DH, DH), buf(led, DH),
            pltpu.VMEM((tokens, DH), F32), pltpu.VMEM((tokens, DH), F32),
            pltpu.VMEM((8, tokens), F32), pltpu.VMEM((peers, 8, tokens), F32),
            pltpu.VMEM((tokens, DH), F32), pltpu.VMEM((tokens, DH), F32),
            *scan, *scan,
            dma((4, heads)), dma((2, peers)),
        ],
        compiler_params=pltpu.CompilerParams(
            collective_id=0, has_side_effects=True, vmem_limit_bytes=32 * 1024 * 1024
        ),
        name="forward_chain",
    )(queries, key_rows, value_rows, grad_out, log_decay, gain)
    grad_q, key_held, value_held, grad_v, grad_k, out, after, cumulative = held
    out, grad_q, grad_k, grad_v = pl.pallas_call(
        functools.partial(last_kernel, chunk),
        out_shape=(rows,) * 4,
        in_specs=[vmem] * 8,
        out_specs=(anywhere,) * 4,
        scratch_shapes=[
            per_head(tokens, DH, dtype=BF16), per_head(tokens, DH, dtype=BF16), dma((4, heads)),
        ],
        compiler_params=pltpu.CompilerParams(vmem_limit_bytes=16 * 1024 * 1024),
        name="last_terms",
    )(key_held, value_held, grad_q, grad_k, grad_v, out, after, cumulative)
    return out, grad_q, grad_k, grad_v, grad_gain.reshape(width)


def solution(mesh):
    in_specs = (
        P("seq", "head"),
        P("seq", "head"),
        P("seq", "head"),
        P("head", "seq"),
        P("head"),
        P("seq", "head"),
    )
    out_specs = (P("seq", "head"), P("seq", "head"), P("seq", "head"), P("seq", "head"), P("head"))
    return jax.shard_map(
        functools.partial(on_device, mesh.shape["seq"], mesh.shape["head"]),
        mesh=mesh, in_specs=in_specs, out_specs=out_specs, check_vma=False,
    )
```

```python
import functools

import jax
import jax.numpy as jnp
from jax import lax
from jax.experimental import pallas as pl
from jax.experimental.pallas import tpu as pltpu
from jax.sharding import PartitionSpec as P

DH = 128
EPSILON = 1e-06
CHUNK = 256
SPLIT_FORWARD = 8
SPLIT_BACKWARD = 8
F32 = jnp.float32
BF16 = jnp.bfloat16
MESH = pl.DeviceIdType.MESH
HIGHEST = lax.Precision.HIGHEST


def mm(left, right, dims):
    return lax.dot_general(left, right, (dims, ((), ())), preferred_element_type=F32)


AB = ((1,), (0,))
ABT = ((1,), (1,))
ATB = ((0,), (0,))


def chunk_cumsum(ld_ref, cum_ref, chunk):
    below = lax.broadcasted_iota(jnp.int32, (chunk, chunk), 0)
    right = lax.broadcasted_iota(jnp.int32, (chunk, chunk), 1)
    tri = (below <= right).astype(F32)
    for j in range(ld_ref.shape[1] // chunk):
        span = slice(j * chunk, (j + 1) * chunk)
        cum_ref[:, span] = lax.dot_general(
            ld_ref[:, span], tri, (AB, ((), ())), precision=HIGHEST, preferred_element_type=F32
        )


def cum_forms(cum_ref, h, j, chunk):
    row = cum_ref[pl.ds(h, 1), j * chunk : (j + 1) * chunk]
    column = jnp.broadcast_to(row, (DH, chunk)).T
    return row, column


def decay_of(row, column):
    chunk = row.shape[1]
    wide = jnp.concatenate([column] * (chunk // DH), axis=1)
    t = lax.broadcasted_iota(jnp.int32, (chunk, chunk), 0)
    s = lax.broadcasted_iota(jnp.int32, (chunk, chunk), 1)
    return jnp.where(t >= s, jnp.exp(wide - row), 0.0)


def remote(src, dst, send, recv, axis, target):
    return pltpu.make_async_remote_copy(
        src_ref=src, dst_ref=dst, send_sem=send, recv_sem=recv,
        device_id={axis: target}, device_id_type=MESH,
    )


def loop(count, body):
    lax.fori_loop(0, count, lambda i, c: (body(i), c)[1], 0)


def wide_loop(count, many, body):
    many = many if count % many == 0 else 1
    loop(count // many, lambda i: [body(many * i + p) for p in range(many)])


def group_loop(count, many, body):
    many = many if count % many == 0 else 1
    loop(count // many, lambda i: body([many * i + p for p in range(many)]))


class Scan:
    def __init__(self, n, reverse, bufs, decays=None):
        (
            self.lsend, self.lrecv, self.own, self.csend, self.arecv, self.asend, self.brecv,
            self.xsend, self.xrecv, self.lsem, self.asend_sem, self.arecv_sem,
            self.bsend_sem, self.brecv_sem, self.xsem,
        ) = bufs
        self.reverse = reverse
        self.chips = n // 2
        self.led = self.lsend.shape[0]
        self.half = self.led * DH // self.chips
        self.parts = DH // self.half
        me = lax.axis_index("seq")
        self.core = lax.rem(me, 2)
        self.chip = me // 2
        self.partner = me + 1 - 2 * self.core
        self.am_first = self.core == (1 if reverse else 0)
        self.mine = self.chip // self.parts
        self.part = lax.rem(self.chip, self.parts)
        self.back = self.half + 8 if reverse else self.half
        self.cross = DH + 8 if reverse else DH
        self.decays = self if decays is None else decays
        self.deep = 4 if self.chips % 4 == 0 else self.chips
        wide = self.chips // self.deep
        distance = lambda d, size: min(d, size - d)
        offsets = [(dx, dz) for dx in range(wide) for dz in range(self.deep)][1:]
        self.order = sorted(offsets, key=lambda o: -distance(o[0], wide) - distance(o[1], self.deep))

    def chip_at(self, dx, dz):
        x = lax.rem(self.chip // self.deep + dx, self.chips // self.deep)
        return x * self.deep + lax.rem(lax.rem(self.chip, self.deep) + dz, self.deep)

    def copy_l(self, j):
        return remote(self.lsend.at[j], self.lrecv.at[j], self.lsem.at[0, j], self.lsem.at[1, j], "seq", self.partner)

    def copy_a(self, j, b, chip):
        return remote(
            self.csend.at[j, b], self.arecv.at[chip], self.asend_sem.at[j, b], self.arecv_sem.at[chip],
            "seq", 2 * (self.parts * j + b) + self.core,
        )

    def copy_b(self, c, j, b):
        rows = pl.ds(0, self.back)
        return remote(
            self.asend.at[c, rows], self.brecv.at[j, b, rows], self.bsend_sem.at[c], self.brecv_sem.at[j, b],
            "seq", 2 * c + self.core,
        )

    def copy_x(self, j):
        rows = pl.ds(0, self.cross)
        return remote(self.xsend.at[j, rows], self.xrecv.at[j, rows], self.xsem.at[0, j], self.xsem.at[1, j], "seq", self.partner)

    def away(self, j, b):
        return self.parts * j + b != self.chip

    def give(self, j, state, extra):
        self.lsend[j, 0:DH] = state
        self.lsend[j, DH : DH + 8] = jnp.broadcast_to(extra, (8, DH))

    def keep(self, j, state, extra):
        self.own[j, 0:DH] = state
        self.own[j, DH : DH + 8] = jnp.broadcast_to(extra, (8, DH))
        self.copy_l(j).wait_recv()
        theirs = self.lrecv[j, 0:DH]
        first = jnp.where(self.am_first, state, theirs)
        second = jnp.where(self.am_first, theirs, state)
        mine, other = self.decays.own[j, DH : DH + 8], self.decays.lrecv[j, DH : DH + 8]
        decay_second = jnp.where(self.am_first, other, mine)[0:1]
        both = decay_second * first + second
        tail = self.own[j, DH : DH + 8] + self.lrecv[j, DH : DH + 8] if self.reverse else mine * other
        for b in range(self.parts):
            self.csend[j, b, 0 : self.half] = both[b * self.half : (b + 1) * self.half]
            self.csend[j, b, self.half : self.half + 8] = tail

            @pl.when(self.away(j, b))
            def _():
                self.copy_a(j, b, self.chip).start()

            @pl.when(jnp.logical_not(self.away(j, b)))
            def _():
                self.arecv[self.chip] = self.csend[j, b]

    def combine(self):
        def arrive(c):
            @pl.when(c != self.chip)
            def _():
                self.copy_a(self.mine, self.part, c).wait_recv()

        if self.reverse:
            loop(self.chips, arrive)
            total = self.arecv[0, self.half : self.half + 8]
            for c in range(1, self.chips):
                total = total + self.arecv[c, self.half : self.half + 8]

        def one(i, state):
            c = self.chips - 1 - i if self.reverse else i
            if not self.reverse:
                arrive(c)
            self.asend[c, 0 : self.half] = state
            if self.reverse:
                self.asend[c, self.half : self.half + 8] = total
            decay = self.decays.arecv[c, self.half : self.half + 1]
            return decay * state + self.arecv[c, 0 : self.half]

        lax.fori_loop(0, self.chips, one, jnp.zeros((self.half, DH), F32))
        for dx, dz in self.order:
            c = self.chip_at(dx, dz)
            self.copy_b(c, self.mine, self.part).start()
        self.brecv[self.mine, self.part, 0 : self.back] = self.asend[self.chip, 0 : self.back]

    def take(self, j, state_ref):
        for b in range(self.parts):
            @pl.when(self.away(j, b))
            def _():
                self.copy_b(self.chip, j, b).wait_recv()

        base = jnp.concatenate([self.brecv[j, b, 0 : self.half] for b in range(self.parts)], axis=0)
        decay = jnp.where(self.am_first, self.decays.own[j, DH : DH + 8], self.decays.lrecv[j, DH : DH + 8])[0:1]
        held = jnp.where(self.am_first, self.own[j, 0:DH], self.lrecv[j, 0:DH])
        after = decay * base + held
        state_ref[...] = jnp.where(self.am_first, base, after)
        self.xsend[j, 0:DH] = jnp.where(self.am_first, after, base)
        if self.reverse:
            self.xsend[j, DH : DH + 8] = self.brecv[j, 0, self.half : self.half + 8]
        self.copy_x(j).start()

    def finish(self, j):
        self.copy_l(j).wait_send()
        self.copy_x(j).wait_send()
        for b in range(self.parts):
            @pl.when(self.away(j, b))
            def _():
                self.copy_a(j, b, self.chip).wait_send()

    def finish_chips(self):
        for dx, dz in self.order:
            self.copy_b(self.chip_at(dx, dz), self.mine, self.part).wait_send()


def main_kernel(
    n, peers, chunk,
    q_hbm, k_hbm, v_hbm, g_hbm, ld_ref, gain_ref,
    q, kd, vd, g, gk, obuf, r_out, etot_ref, gg_out, lc,
    k, v, qd, att, cum_ref, s_out, state_in, sq_acc, in_acc,
    stat_send, stat_recv, inv_b, cen_b, gain_acc, *rest,
):
    load_sem, stat_sem = rest[-2:]
    bufs1, bufs2 = rest[:15], rest[15:30]
    heads, tokens, _ = q.shape
    chunks = tokens // chunk
    me = lax.axis_index("seq")
    my_head = lax.axis_index("head")
    columns = heads * DH * peers

    def load(i, hbm, vmem, h):
        where = pl.ds(pl.multiple_of(h * DH, DH), DH)
        return pltpu.make_async_copy(hbm.at[:, where], vmem.at[h], load_sem.at[i, h])

    def load_kv(h):
        load(0, k_hbm, k, h).start()
        load(1, v_hbm, v, h).start()

    def load_q(h):
        load(2, q_hbm, q, h).start()

    def load_g(h):
        load(3, g_hbm, g, h).start()

    barrier = pltpu.get_barrier_semaphore()
    for off in range(1, n // 2):
        pl.semaphore_signal(barrier, inc=1, device_id={"seq": lax.rem(me + 2 * off, n)}, device_id_type=MESH)
    pl.semaphore_signal(barrier, inc=1, device_id={"seq": me + 1 - 2 * lax.rem(me, 2)}, device_id_type=MESH)
    for off in range(1, peers):
        pl.semaphore_signal(barrier, inc=1, device_id={"head": lax.rem(my_head + off, peers)}, device_id_type=MESH)


    forward = Scan(n, False, bufs1)
    backward = Scan(n, True, bufs2, forward)
    core, led = forward.core, forward.led

    def led_head(j):
        return 2 * j + core

    def other_head(j):
        return 2 * j + 1 - core

    def turned(i):
        far = led // 2 + lax.rem(i, 2) * 2 * ((i + 1) // 2) - (i + 1) // 2
        return lax.rem(far + forward.mine, led)

    loop(led, lambda j: load_kv(other_head(j)))
    loop(led, lambda i: load_kv(led_head(turned(i))))
    chunk_cumsum(ld_ref, cum_ref, chunk)
    for j in range(chunks):
        end = (j + 1) * chunk
        etot_ref[j] = jnp.exp(jnp.broadcast_to(cum_ref[:, end - 1 : end], (heads, DH)))

    def total_of(h, j):
        return etot_ref[j, pl.ds(h, 1)]

    def local_state(h):
        load(0, k_hbm, k, h).wait()
        load(1, v_hbm, v, h).wait()
        state = decay = None
        for j in range(chunks):
            span = slice(j * chunk, (j + 1) * chunk)
            _, column = cum_forms(cum_ref, h, j, chunk)
            tail = jnp.exp(column[chunk - 1 : chunk, :] - column)
            faded = (k[h, span].astype(F32) * tail).astype(BF16)
            kd[h, span] = faded
            part = mm(faded, v[h, span], ATB)
            lc[h, j] = part
            total = total_of(h, j)
            state = part if j == 0 else total * state + part
            decay = total if j == 0 else decay * total
        return state, decay

    def give_forward(j):
        forward.give(j, *local_state(other_head(j)))

    def keep_forward(i):
        j = turned(i)
        forward.keep(j, *local_state(led_head(j)))

    loop(led, give_forward)
    pl.semaphore_wait(barrier, n // 2 - 1 + 1 + peers - 1)
    loop(led, lambda j: forward.copy_l(j).start())
    loop(heads, load_q)
    loop(heads, load_g)
    loop(led, keep_forward)

    def intra(h):
        load(2, q_hbm, q, h).wait()
        for j in range(chunks):
            span = slice(j * chunk, (j + 1) * chunk)
            row, column = cum_forms(cum_ref, h, j, chunk)
            scores = mm(q[h, span], k[h, span], ABT)
            weights = (scores * decay_of(row, column)).astype(BF16)
            att[h, span] = mm(weights, v[h, span], AB)
            qd[h, span] = (q[h, span].astype(F32) * jnp.exp(column)).astype(BF16)
            tail = jnp.exp(column[chunk - 1 : chunk, :] - column)
            vd[h, span] = (v[h, span].astype(F32) * tail).astype(BF16)

    wide_loop(SPLIT_FORWARD, 2, intra)
    forward.combine()
    wide_loop(heads - SPLIT_FORWARD, 2, lambda i: intra(i + SPLIT_FORWARD))
    sq_acc[...] = jnp.zeros_like(sq_acc)
    in_acc[...] = jnp.zeros_like(in_acc)

    gain_acc[...] = jnp.zeros_like(gain_acc)
    loop(heads, lambda h: load(3, g_hbm, g, h).wait())

    def spread(h, state):
        for j in range(chunks):
            s_out[h, j] = state.astype(BF16)
            if j < chunks - 1:
                state = total_of(h, j) * state + lc[h, j]

    def inter(j, pair):
        span = slice(j * chunk, (j + 1) * chunk)
        square = inner = None
        for h in pair:
            whole = att[h, span] + mm(qd[h, span], s_out[h, j], AB)
            att[h, span] = whole
            scaled = g[h, span].astype(F32) * gain_ref[pl.ds(h, 1), :]
            square = whole * whole if square is None else square + whole * whole
            inner = scaled * whole if inner is None else inner + scaled * whole
        sq_acc[span] += square
        in_acc[span] += inner

    ones = jnp.ones((8, DH), F32)

    def row_sums(acc):
        return lax.dot_general(ones, acc, (ABT, ((), ())), precision=HIGHEST, preferred_element_type=F32)

    upper = lax.broadcasted_iota(jnp.int32, (8, chunk), 0) < 4

    def stat_copy(j, off, slot):
        return remote(
            stat_send.at[j], stat_recv.at[j, slot], stat_sem.at[0, j, off], stat_sem.at[1, j, off],
            "head", lax.rem(my_head + off, peers),
        )

    def send_stats(j):
        span = slice(j * chunk, (j + 1) * chunk)
        stat_send[j] = jnp.where(upper, row_sums(sq_acc[span]), row_sums(in_acc[span]))
        for off in range(1, peers):
            stat_copy(j, off, my_head).start()
        stat_recv[j, my_head] = stat_send[j]

    def take_forward(j):
        forward.take(j, state_in.at[j])
        spread(led_head(j), state_in[j])

    def take_other_forward(j):
        forward.copy_x(j).wait_recv()
        spread(other_head(j), forward.xrecv[j, 0:DH])

    loop(led, take_forward)
    group_loop(led, 4, lambda js: inter(0, [led_head(j) for j in js]))
    loop(led, take_other_forward)
    group_loop(led, 4, lambda js: inter(0, [other_head(j) for j in js]))
    send_stats(0)
    for j in range(1, chunks):
        group_loop(heads, 8, functools.partial(inter, j))
        send_stats(j)

    def take_stats(j):
        span = slice(j * chunk, (j + 1) * chunk)
        for off in range(1, peers):
            stat_copy(j, off, lax.rem(my_head + peers - off, peers)).wait_recv()
        stats = stat_recv[j, 0]
        for i in range(1, peers):
            stats = stats + stat_recv[j, i]
        inverse = lax.rsqrt(stats[0:1] / columns + EPSILON)
        center = stats[4:5] * inverse / columns
        inv_b[span] = jnp.broadcast_to(inverse, (DH, chunk)).T
        cen_b[span] = jnp.broadcast_to(inverse * inverse * center, (DH, chunk)).T

    def normalize(j, h):
        span = slice(j * chunk, (j + 1) * chunk)
        gain = gain_ref[pl.ds(h, 1), :]
        whole = att[h, span]
        normed = whole * inv_b[span]
        obuf[h, span] = (normed * gain).astype(BF16)
        cotangent = g[h, span].astype(F32)
        product = cotangent * normed
        gain_acc[h] += jnp.sum(product.reshape(chunk // 8, 8, DH), axis=0)
        grad = (inv_b[span] * (cotangent * gain) - whole * cen_b[span]).astype(BF16)
        g[h, span] = grad
        return mm(qd[h, span], grad, ATB)

    def normalize_early(j, h):
        lc[h, j] = normalize(j, h)

    for j in range(chunks - 1):
        take_stats(j)
        wide_loop(heads, 8, functools.partial(normalize_early, j))
    take_stats(chunks - 1)

    def normalize_last(h):
        state = normalize(chunks - 1, h)
        lc[h, chunks - 1] = state
        for j in reversed(range(chunks - 1)):
            state = total_of(h, j) * state + lc[h, j]
        return state, gain_acc[h]

    def give_backward(j):
        backward.give(j, *normalize_last(other_head(j)))
        backward.copy_l(j).start()

    def keep_backward(i):
        j = turned(i)
        backward.keep(j, *normalize_last(led_head(j)))

    loop(led, give_backward)
    loop(led, keep_backward)

    def gradients(h):
        for j in range(chunks):
            span = slice(j * chunk, (j + 1) * chunk)
            row, column = cum_forms(cum_ref, h, j, chunk)
            decay = decay_of(row, column)
            queries, keys, values, grad = q[h, span], k[h, span], v[h, span], g[h, span]
            weights = (mm(queries, keys, ABT) * decay).astype(BF16)
            grad_weights = (mm(grad, values, ABT) * decay).astype(BF16)
            q[h, span] = (
                mm(grad_weights, keys, AB) + jnp.exp(column) * mm(grad, s_out[h, j], ABT)
            ).astype(BF16)
            gk[h, span] = mm(grad_weights, queries, ATB).astype(BF16)
            g[h, span] = mm(weights, grad, ATB).astype(BF16)

    wide_loop(SPLIT_BACKWARD, 2, gradients)
    backward.combine()
    wide_loop(heads - SPLIT_BACKWARD, 2, lambda i: gradients(i + SPLIT_BACKWARD))
    def take_led(j):
        h = led_head(j)
        backward.take(j, r_out.at[h])
        gg_out[pl.ds(h, 1), :] = jnp.sum(backward.xsend[j, DH : DH + 8], axis=0, keepdims=True)

    def take_other(j):
        h = other_head(j)
        backward.copy_x(j).wait_recv()
        r_out[h] = backward.xrecv[j, 0:DH]
        gg_out[pl.ds(h, 1), :] = jnp.sum(backward.xrecv[j, DH : DH + 8], axis=0, keepdims=True)

    loop(led, take_led)
    loop(led, take_other)

    def finish(j):
        forward.finish(j)
        backward.finish(j)

    loop(led, finish)
    forward.finish_chips()
    backward.finish_chips()
    for j in range(chunks):
        for off in range(1, peers):
            stat_copy(j, off, my_head).wait_send()


def last_kernel(
    chunk, kd, vd, gq, gk, gv, out, after, etot_ref, lc,
    out_hbm, gq_hbm, gk_hbm, gv_hbm, k_stage, v_stage, store_sem,
):
    heads, tokens, _ = kd.shape

    def store(i, vmem, hbm, h):
        where = pl.ds(pl.multiple_of(h * DH, DH), DH)
        return pltpu.make_async_copy(vmem.at[h], hbm.at[:, where], store_sem.at[i, h])

    def copies(h):
        return (
            store(0, out, out_hbm, h), store(1, gq, gq_hbm, h),
            store(2, k_stage, gk_hbm, h), store(3, v_stage, gv_hbm, h),
        )

    def first(h):
        ready = copies(h)
        ready[0].start()
        ready[1].start()

    def one(h):
        ready = copies(h)
        state = after[h]
        for j in reversed(range(tokens // chunk)):
            span = slice(j * chunk, (j + 1) * chunk)
            rounded = state.astype(BF16)
            k_stage[h, span] = (gk[h, span].astype(F32) + mm(vd[h, span], rounded, ABT)).astype(BF16)
            v_stage[h, span] = (gv[h, span].astype(F32) + mm(kd[h, span], rounded, AB)).astype(BF16)
            if j > 0:
                state = etot_ref[j, pl.ds(h, 1)] * state + lc[h, j]
        ready[2].start()
        ready[3].start()

    def wait(h):
        for copy in copies(h):
            copy.wait()

    loop(heads, first)
    loop(heads, one)
    loop(heads, wait)


def on_device(n, peers, queries, key_rows, value_rows, log_decay, norm_gain, grad_out):
    tokens, width = queries.shape
    heads = width // DH
    chunk = CHUNK if tokens % CHUNK == 0 else tokens
    chunks = tokens // chunk
    gain = norm_gain.reshape(heads, DH)
    anywhere = pl.BlockSpec(memory_space=pl.ANY)
    vmem = pl.BlockSpec(memory_space=pltpu.VMEM)
    rows = jax.ShapeDtypeStruct((tokens, width), BF16)
    states = jax.ShapeDtypeStruct((heads, chunks, DH, DH), BF16)
    per_head = lambda *shape, dtype=F32: pltpu.VMEM((heads, *shape), dtype)
    dma = pltpu.SemaphoreType.DMA
    led, chips = heads // 2, n // 2
    half = led * DH // chips
    parts = DH // half
    buf = lambda *shape: pltpu.VMEM((*shape, DH), F32)
    scan = [
        buf(led, DH + 8), buf(led, DH + 8), buf(led, DH + 8), buf(led, parts, half + 8),
        buf(chips, half + 8), buf(chips, half + 8), buf(led, parts, half + 8),
        buf(led, DH + 8), buf(led, DH + 8),
        dma((2, led)), dma((led, parts)), dma((chips,)), dma((chips,)), dma((led, parts)), dma((2, led)),
    ]
    by_head = lambda dtype: pltpu.VMEM((heads, tokens, DH), dtype)
    *held, grad_gain, state_grads = pl.pallas_call(
        functools.partial(main_kernel, n, peers, chunk),
        out_shape=(
            *[by_head(BF16)] * 6,
            pltpu.VMEM((heads, DH, DH), F32), pltpu.VMEM((chunks, heads, DH), F32),
            jax.ShapeDtypeStruct((heads, DH), F32), pltpu.VMEM((heads, chunks, DH, DH), F32),
        ),
        in_specs=[anywhere] * 4 + [vmem] * 2,
        out_specs=(vmem,) * 10,
        scratch_shapes=[
            by_head(BF16), by_head(BF16), by_head(BF16), by_head(F32), pltpu.VMEM((heads, tokens), F32),
            per_head(chunks, DH, DH, dtype=BF16), buf(led, DH),
            pltpu.VMEM((tokens, DH), F32), pltpu.VMEM((tokens, DH), F32),
            pltpu.VMEM((chunks, 8, chunk), F32), pltpu.VMEM((chunks, peers, 8, chunk), F32),
            pltpu.VMEM((tokens, DH), F32), pltpu.VMEM((tokens, DH), F32), per_head(8, DH),
            *scan, *scan,
            dma((4, heads)), dma((2, chunks, peers)),
        ],
        compiler_params=pltpu.CompilerParams(
            collective_id=0, has_side_effects=True, vmem_limit_bytes=36 * 1024 * 1024
        ),
        name="forward_chain",
    )(queries, key_rows, value_rows, grad_out, log_decay, gain)
    grad_q, key_faded, value_faded, grad_v, grad_k, out, after, totals = held
    out, grad_q, grad_k, grad_v = pl.pallas_call(
        functools.partial(last_kernel, chunk),
        out_shape=(rows,) * 4,
        in_specs=[vmem] * 9,
        out_specs=(anywhere,) * 4,
        scratch_shapes=[
            per_head(tokens, DH, dtype=BF16), per_head(tokens, DH, dtype=BF16), dma((4, heads)),
        ],
        compiler_params=pltpu.CompilerParams(vmem_limit_bytes=10 * 1024 * 1024),
        name="last_terms",
    )(key_faded, value_faded, grad_q, grad_k, grad_v, out, after, totals, state_grads)
    return out, grad_q, grad_k, grad_v, grad_gain.reshape(width)


def solution(mesh):
    in_specs = (
        P("seq", "head"),
        P("seq", "head"),
        P("seq", "head"),
        P("head", "seq"),
        P("head"),
        P("seq", "head"),
    )
    out_specs = (P("seq", "head"), P("seq", "head"), P("seq", "head"), P("seq", "head"), P("head"))
    return jax.shard_map(
        functools.partial(on_device, mesh.shape["seq"], mesh.shape["head"]),
        mesh=mesh, in_specs=in_specs, out_specs=out_specs, check_vma=False,
    )
```

```python
import functools

import jax
import jax.numpy as jnp
from jax import lax
from jax.experimental import pallas as pl
from jax.experimental.pallas import tpu as pltpu
from jax.sharding import PartitionSpec as P

DH = 128
EPSILON = 1e-06
CHUNK = 256
GROUPS = 1
SPLIT_FORWARD = (8,)
SPLIT_BACKWARD = (8,)
F32 = jnp.float32
BF16 = jnp.bfloat16
MESH = pl.DeviceIdType.MESH
HIGHEST = lax.Precision.HIGHEST


def mm(left, right, dims):
    return lax.dot_general(left, right, (dims, ((), ())), preferred_element_type=F32)


AB = ((1,), (0,))
ABT = ((1,), (1,))
ATB = ((0,), (0,))


def chunk_cumsum(ld_ref, cum_ref, chunk):
    below = lax.broadcasted_iota(jnp.int32, (chunk, chunk), 0)
    right = lax.broadcasted_iota(jnp.int32, (chunk, chunk), 1)
    tri = (below <= right).astype(F32)
    for j in range(ld_ref.shape[1] // chunk):
        span = slice(j * chunk, (j + 1) * chunk)
        cum_ref[:, span] = lax.dot_general(
            ld_ref[:, span], tri, (AB, ((), ())), precision=HIGHEST, preferred_element_type=F32
        )


def cum_forms(cum_ref, h, j, chunk):
    row = cum_ref[pl.ds(h, 1), j * chunk : (j + 1) * chunk]
    column = jnp.broadcast_to(row, (DH, chunk)).T
    return row, column


def decay_of(row, column):
    chunk = row.shape[1]
    wide = jnp.concatenate([column] * (chunk // DH), axis=1)
    t = lax.broadcasted_iota(jnp.int32, (chunk, chunk), 0)
    s = lax.broadcasted_iota(jnp.int32, (chunk, chunk), 1)
    return jnp.where(t >= s, jnp.exp(wide - row), 0.0)


def remote(src, dst, send, recv, axis, target):
    return pltpu.make_async_remote_copy(
        src_ref=src, dst_ref=dst, send_sem=send, recv_sem=recv,
        device_id={axis: target}, device_id_type=MESH,
    )


def loop(count, body):
    lax.fori_loop(0, count, lambda i, c: (body(i), c)[1], 0)


def wide_loop(count, many, body):
    many = many if count % many == 0 else 1
    loop(count // many, lambda i: [body(many * i + p) for p in range(many)])


def group_loop(count, many, body):
    many = many if count % many == 0 else 1
    loop(count // many, lambda i: body([many * i + p for p in range(many)]))


class Scan:
    def __init__(self, n, reverse, base, bufs, decays=None):
        (
            self.lsend, self.lrecv, self.own, self.csend, self.arecv, self.asend, self.brecv,
            self.xsend, self.xrecv, self.lsem, self.asend_sem, self.arecv_sem,
            self.bsend_sem, self.brecv_sem, self.xsem,
        ) = bufs
        self.reverse = reverse
        self.base = base
        self.chips = n // 2
        self.led = self.lsend.shape[0]
        self.half = self.led * DH // self.chips
        self.parts = DH // self.half
        me = lax.axis_index("seq")
        self.core = lax.rem(me, 2)
        self.chip = me // 2
        self.partner = me + 1 - 2 * self.core
        self.am_first = self.core == (1 if reverse else 0)
        self.mine = self.chip // self.parts
        self.part = lax.rem(self.chip, self.parts)
        self.back = self.half + 1 if reverse else self.half
        self.cross = DH + 1 if reverse else DH
        self.decays = self if decays is None else decays
        self.deep = 4 if self.chips % 4 == 0 else self.chips
        wide = self.chips // self.deep
        distance = lambda d, size: min(d, size - d)
        offsets = [(dx, dz) for dx in range(wide) for dz in range(self.deep)][1:]
        self.order = sorted(offsets, key=lambda o: -distance(o[0], wide) - distance(o[1], self.deep))

    def led_head(self, j):
        return self.base + 2 * j + self.core

    def other_head(self, j):
        return self.base + 2 * j + 1 - self.core

    def turned(self, i):
        far = self.led // 2 + lax.rem(i, 2) * 2 * ((i + 1) // 2) - (i + 1) // 2
        return lax.rem(far + self.mine, self.led)

    def chip_at(self, dx, dz):
        x = lax.rem(self.chip // self.deep + dx, self.chips // self.deep)
        return x * self.deep + lax.rem(lax.rem(self.chip, self.deep) + dz, self.deep)

    def copy_l(self, j):
        return remote(self.lsend.at[j], self.lrecv.at[j], self.lsem.at[0, j], self.lsem.at[1, j], "seq", self.partner)

    def copy_a(self, j, b, chip):
        return remote(
            self.csend.at[j, b, pl.ds(0, self.half + 1)], self.arecv.at[chip, pl.ds(0, self.half + 1)], self.asend_sem.at[j, b], self.arecv_sem.at[chip],
            "seq", 2 * (self.parts * j + b) + self.core,
        )

    def copy_b(self, c, j, b):
        rows = pl.ds(0, self.back)
        return remote(
            self.asend.at[c, rows], self.brecv.at[j, b, rows], self.bsend_sem.at[c], self.brecv_sem.at[j, b],
            "seq", 2 * c + self.core,
        )

    def copy_x(self, j):
        rows = pl.ds(0, self.cross)
        return remote(self.xsend.at[j, rows], self.xrecv.at[j, rows], self.xsem.at[0, j], self.xsem.at[1, j], "seq", self.partner)

    def away(self, j, b):
        return self.parts * j + b != self.chip

    def give(self, j, state, extra):
        self.lsend[j, 0:DH] = state
        self.lsend[j, DH : DH + 8] = jnp.broadcast_to(extra, (8, DH))

    def keep(self, j, state, extra):
        self.own[j, 0:DH] = state
        self.own[j, DH : DH + 8] = jnp.broadcast_to(extra, (8, DH))
        self.copy_l(j).wait_recv()
        theirs = self.lrecv[j, 0:DH]
        first = jnp.where(self.am_first, state, theirs)
        second = jnp.where(self.am_first, theirs, state)
        mine, other = self.decays.own[j, DH : DH + 8], self.decays.lrecv[j, DH : DH + 8]
        decay_second = jnp.where(self.am_first, other, mine)[0:1]
        both = decay_second * first + second
        if self.reverse:
            tail = jnp.sum(self.own[j, DH : DH + 8] + self.lrecv[j, DH : DH + 8], axis=0, keepdims=True)
        else:
            tail = (mine * other)[0:1]
        for b in range(self.parts):
            self.csend[j, b, 0 : self.half] = both[b * self.half : (b + 1) * self.half]
            self.csend[j, b, self.half : self.half + 8] = jnp.broadcast_to(tail, (8, DH))
        for step in range(self.parts):
            b = lax.rem(self.part + self.parts // 2 + step, self.parts)

            @pl.when(self.away(j, b))
            def _():
                self.copy_a(j, b, self.chip).start()

            @pl.when(jnp.logical_not(self.away(j, b)))
            def _():
                self.arecv[self.chip] = self.csend[j, b]

    def combine(self):
        def arrive(c):
            @pl.when(c != self.chip)
            def _():
                self.copy_a(self.mine, self.part, c).wait_recv()

        if self.reverse:
            loop(self.chips, arrive)
            total = self.arecv[0, self.half : self.half + 1]
            for c in range(1, self.chips):
                total = total + self.arecv[c, self.half : self.half + 1]
            total = jnp.broadcast_to(total, (8, DH))

        def one(i, state):
            c = self.chips - 1 - i if self.reverse else i
            if not self.reverse:
                arrive(c)
            self.asend[c, 0 : self.half] = state
            if self.reverse:
                self.asend[c, self.half : self.half + 8] = total
            decay = self.decays.arecv[c, self.half : self.half + 1]
            return decay * state + self.arecv[c, 0 : self.half]

        lax.fori_loop(0, self.chips, one, jnp.zeros((self.half, DH), F32))
        for dx, dz in self.order:
            c = self.chip_at(dx, dz)
            self.copy_b(c, self.mine, self.part).start()
        self.brecv[self.mine, self.part, 0 : self.half] = self.asend[self.chip, 0 : self.half]
        if self.reverse:
            self.brecv[self.mine, self.part, self.half : self.half + 1] = self.asend[self.chip, self.half : self.half + 1]

    def take(self, j, state_ref):
        for b in range(self.parts):
            @pl.when(self.away(j, b))
            def _():
                self.copy_b(self.chip, j, b).wait_recv()

        base = jnp.concatenate([self.brecv[j, b, 0 : self.half] for b in range(self.parts)], axis=0)
        decay = jnp.where(self.am_first, self.decays.own[j, DH : DH + 8], self.decays.lrecv[j, DH : DH + 8])[0:1]
        held = jnp.where(self.am_first, self.own[j, 0:DH], self.lrecv[j, 0:DH])
        after = decay * base + held
        state_ref[...] = jnp.where(self.am_first, base, after)
        self.xsend[j, 0:DH] = jnp.where(self.am_first, after, base)
        if self.reverse:
            self.xsend[j, DH : DH + 1] = self.brecv[j, 0, self.half : self.half + 1]
        self.copy_x(j).start()

    def finish(self, j):
        self.copy_l(j).wait_send()
        self.copy_x(j).wait_send()
        for b in range(self.parts):
            @pl.when(self.away(j, b))
            def _():
                self.copy_a(j, b, self.chip).wait_send()

    def finish_chips(self):
        for dx, dz in self.order:
            self.copy_b(self.chip_at(dx, dz), self.mine, self.part).wait_send()


def main_kernel(
    n, peers, chunk,
    q_hbm, k_hbm, v_hbm, g_hbm, ld_hbm, gain_hbm,
    q, kd, vd, g, gk, obuf, r_out, etot_ref, gg_out, lc,
    k, v, qd, att, cum_ref, s_out, state_in, sq_acc, in_acc,
    stat_send, stat_recv, inv_b, cen_b, gain_acc, *rest,
):
    ld_ref, gain_ref, load_sem, stat_sem, small_sem = rest[-5:]
    bufs = [rest[15 * i : 15 * (i + 1)] for i in range(2 * GROUPS)]
    heads, tokens, _ = q.shape
    chunks = tokens // chunk
    me = lax.axis_index("seq")
    my_head = lax.axis_index("head")
    columns = heads * DH * peers

    def load(i, hbm, vmem, h):
        where = pl.ds(pl.multiple_of(h * DH, DH), DH)
        return pltpu.make_async_copy(hbm.at[:, where], vmem.at[h], load_sem.at[i, h])

    def load_kv(h):
        load(0, k_hbm, k, h).start()
        load(1, v_hbm, v, h).start()

    def load_q(h):
        load(2, q_hbm, q, h).start()

    def load_g(h):
        load(3, g_hbm, g, h).start()

    load_ld = pltpu.make_async_copy(ld_hbm, ld_ref, small_sem.at[0])
    load_gain = pltpu.make_async_copy(gain_hbm, gain_ref, small_sem.at[1])
    load_ld.start()
    load_gain.start()
    barrier = pltpu.get_barrier_semaphore()
    for off in range(1, n // 2):
        pl.semaphore_signal(barrier, inc=1, device_id={"seq": lax.rem(me + 2 * off, n)}, device_id_type=MESH)
    pl.semaphore_signal(barrier, inc=1, device_id={"seq": me + 1 - 2 * lax.rem(me, 2)}, device_id_type=MESH)
    for off in range(1, peers):
        pl.semaphore_signal(barrier, inc=1, device_id={"head": lax.rem(my_head + off, peers)}, device_id_type=MESH)


    each = heads // GROUPS
    forward = [Scan(n, False, i * each, bufs[i]) for i in range(GROUPS)]
    backward = [Scan(n, True, i * each, bufs[GROUPS + i], forward[i]) for i in range(GROUPS)]
    led = each // 2

    for scan in forward:
        loop(led, lambda j, scan=scan: load_kv(scan.other_head(j)))
        loop(led, lambda i, scan=scan: load_kv(scan.led_head(scan.turned(i))))
    load_ld.wait()
    load_gain.wait()
    chunk_cumsum(ld_ref, cum_ref, chunk)
    for j in range(chunks):
        end = (j + 1) * chunk
        etot_ref[j] = jnp.exp(jnp.broadcast_to(cum_ref[:, end - 1 : end], (heads, DH)))

    def total_of(h, j):
        return etot_ref[j, pl.ds(h, 1)]

    def local_state(h):
        load(0, k_hbm, k, h).wait()
        load(1, v_hbm, v, h).wait()
        state = decay = None
        for j in range(chunks):
            span = slice(j * chunk, (j + 1) * chunk)
            _, column = cum_forms(cum_ref, h, j, chunk)
            tail = jnp.exp(column[chunk - 1 : chunk, :] - column)
            faded = (k[h, span].astype(F32) * tail).astype(BF16)
            kd[h, span] = faded
            part = mm(faded, v[h, span], ATB)
            lc[h, j] = part
            total = total_of(h, j)
            state = part if j == 0 else total * state + part
            decay = total if j == 0 else decay * total
        return state, decay

    for i, scan in enumerate(forward):
        def give_forward(j, scan=scan):
            scan.give(j, *local_state(scan.other_head(j)))

        def keep_forward(i, scan=scan):
            j = scan.turned(i)
            scan.keep(j, *local_state(scan.led_head(j)))

        loop(led, give_forward)
        if i == 0:
            pl.semaphore_wait(barrier, n // 2 - 1 + 1 + peers - 1)
        loop(led, lambda j, scan=scan: scan.copy_l(j).start())
        loop(led, keep_forward)
    loop(heads, load_q)
    loop(heads, load_g)

    def intra(h):
        load(2, q_hbm, q, h).wait()
        for j in range(chunks):
            span = slice(j * chunk, (j + 1) * chunk)
            row, column = cum_forms(cum_ref, h, j, chunk)
            scores = mm(q[h, span], k[h, span], ABT)
            weights = (scores * decay_of(row, column)).astype(BF16)
            att[h, span] = mm(weights, v[h, span], AB)
            qd[h, span] = (q[h, span].astype(F32) * jnp.exp(column)).astype(BF16)
            tail = jnp.exp(column[chunk - 1 : chunk, :] - column)
            vd[h, span] = (v[h, span].astype(F32) * tail).astype(BF16)

    def between(splits, scans, body):
        edges = (0, *splits, heads)
        for i, (low, high) in enumerate(zip(edges, edges[1:])):
            wide_loop(high - low, 2, lambda h, low=low: body(h + low))
            if i < len(scans):
                scans[i].combine()

    between(SPLIT_FORWARD, forward, intra)

    sq_acc[...] = jnp.zeros_like(sq_acc)
    in_acc[...] = jnp.zeros_like(in_acc)

    gain_acc[...] = jnp.zeros_like(gain_acc)
    loop(heads, lambda h: load(3, g_hbm, g, h).wait())

    def spread(h, state):
        for j in range(chunks):
            s_out[h, j] = state.astype(BF16)
            if j < chunks - 1:
                state = total_of(h, j) * state + lc[h, j]

    def inter(j, pair):
        span = pl.ds(j * chunk if isinstance(j, int) else pl.multiple_of(j * chunk, chunk), chunk)
        square = inner = None
        for h in pair:
            whole = att[h, span] + mm(qd[h, span], s_out[h, j], AB)
            att[h, span] = whole
            scaled = g[h, span].astype(F32) * gain_ref[pl.ds(h, 1), :]
            square = whole * whole if square is None else square + whole * whole
            inner = scaled * whole if inner is None else inner + scaled * whole
        sq_acc[span] += square
        in_acc[span] += inner

    ones = jnp.ones((8, DH), F32)

    def row_sums(acc):
        return lax.dot_general(ones, acc, (ABT, ((), ())), precision=HIGHEST, preferred_element_type=F32)

    upper = lax.broadcasted_iota(jnp.int32, (8, chunk), 0) < 4

    def stat_copy(j, off, slot):
        return remote(
            stat_send.at[j], stat_recv.at[j, slot], stat_sem.at[0, j, off], stat_sem.at[1, j, off],
            "head", lax.rem(my_head + off, peers),
        )

    def send_stats(j):
        span = slice(j * chunk, (j + 1) * chunk)
        stat_send[j] = jnp.where(upper, row_sums(sq_acc[span]), row_sums(in_acc[span]))
        for off in range(1, peers):
            stat_copy(j, off, my_head).start()
        stat_recv[j, my_head] = stat_send[j]

    for i, scan in enumerate(forward):
        def take_forward(j, scan=scan):
            scan.take(j, state_in.at[j])
            spread(scan.led_head(j), state_in[j])

        def take_other_forward(j, scan=scan):
            scan.copy_x(j).wait_recv()
            spread(scan.other_head(j), scan.xrecv[j, 0:DH])

        everyone = [scan.base + h for h in range(each)]
        loop(led, take_forward)
        if i < GROUPS - 1:
            loop(led, take_other_forward)
            loop(chunks, lambda j, everyone=everyone: inter(j, everyone))
            continue
        inter(0, [scan.led_head(j) for j in range(led)])
        loop(led, take_other_forward)
        inter(0, [scan.other_head(j) for j in range(led)])
        send_stats(0)
        for j in range(1, chunks):
            inter(j, everyone)
            send_stats(j)

    def take_stats(j):
        span = slice(j * chunk, (j + 1) * chunk)
        for off in range(1, peers):
            stat_copy(j, off, lax.rem(my_head + peers - off, peers)).wait_recv()
        stats = stat_recv[j, 0]
        for i in range(1, peers):
            stats = stats + stat_recv[j, i]
        inverse = lax.rsqrt(stats[0:1] / columns + EPSILON)
        center = stats[4:5] * inverse / columns
        inv_b[span] = jnp.broadcast_to(inverse, (DH, chunk)).T
        cen_b[span] = jnp.broadcast_to(inverse * inverse * center, (DH, chunk)).T

    def normalize(j, h):
        span = slice(j * chunk, (j + 1) * chunk)
        gain = gain_ref[pl.ds(h, 1), :]
        whole = att[h, span]
        normed = whole * inv_b[span]
        obuf[h, span] = (normed * gain).astype(BF16)
        cotangent = g[h, span].astype(F32)
        product = cotangent * normed
        gain_acc[h] += jnp.sum(product.reshape(chunk // 8, 8, DH), axis=0)
        grad = (inv_b[span] * (cotangent * gain) - whole * cen_b[span]).astype(BF16)
        g[h, span] = grad
        return mm(qd[h, span], grad, ATB)

    def normalize_early(j, h):
        lc[h, j] = normalize(j, h)

    for j in range(chunks - 1):
        take_stats(j)
        wide_loop(heads, 8, functools.partial(normalize_early, j))
    take_stats(chunks - 1)

    def normalize_last(h):
        state = normalize(chunks - 1, h)
        lc[h, chunks - 1] = state
        for j in reversed(range(chunks - 1)):
            state = total_of(h, j) * state + lc[h, j]
        return state, gain_acc[h]

    for scan in backward:
        def give_backward(j, scan=scan):
            scan.give(j, *normalize_last(scan.other_head(j)))
            scan.copy_l(j).start()

        def keep_backward(i, scan=scan):
            j = scan.turned(i)
            scan.keep(j, *normalize_last(scan.led_head(j)))

        loop(led, give_backward)
        loop(led, keep_backward)

    def gradients(h):
        for j in range(chunks):
            span = slice(j * chunk, (j + 1) * chunk)
            row, column = cum_forms(cum_ref, h, j, chunk)
            decay = decay_of(row, column)
            queries, keys, values, grad = q[h, span], k[h, span], v[h, span], g[h, span]
            weights = (mm(queries, keys, ABT) * decay).astype(BF16)
            grad_weights = (mm(grad, values, ABT) * decay).astype(BF16)
            q[h, span] = (
                mm(grad_weights, keys, AB) + jnp.exp(column) * mm(grad, s_out[h, j], ABT)
            ).astype(BF16)
            gk[h, span] = mm(grad_weights, queries, ATB).astype(BF16)
            g[h, span] = mm(weights, grad, ATB).astype(BF16)

    between(SPLIT_BACKWARD, backward, gradients)

    for scan in backward:
        def take_led(j, scan=scan):
            h = scan.led_head(j)
            scan.take(j, r_out.at[h])
            gg_out[pl.ds(h, 1), :] = scan.xsend[j, DH : DH + 1]

        loop(led, take_led)

    for scan in backward:
        def take_other(j, scan=scan):
            h = scan.other_head(j)
            scan.copy_x(j).wait_recv()
            r_out[h] = scan.xrecv[j, 0:DH]
            gg_out[pl.ds(h, 1), :] = scan.xrecv[j, DH : DH + 1]

        loop(led, take_other)

    for scan in forward + backward:
        loop(led, scan.finish)
        scan.finish_chips()
    for j in range(chunks):
        for off in range(1, peers):
            stat_copy(j, off, my_head).wait_send()


def last_kernel(
    chunk, kd, vd, gq, gk, gv, out, after, etot_ref, lc, gg,
    out_hbm, gq_hbm, gk_hbm, gv_hbm, gg_hbm, k_stage, v_stage, store_sem, gain_sem,
):
    heads, tokens, _ = kd.shape

    def store(i, vmem, hbm, h):
        where = pl.ds(pl.multiple_of(h * DH, DH), DH)
        return pltpu.make_async_copy(vmem.at[h], hbm.at[:, where], store_sem.at[i, h])

    def copies(h):
        return (
            store(0, out, out_hbm, h), store(1, gq, gq_hbm, h),
            store(2, k_stage, gk_hbm, h), store(3, v_stage, gv_hbm, h),
        )

    def first(h):
        ready = copies(h)
        ready[0].start()
        ready[1].start()

    def one(h):
        ready = copies(h)
        state = after[h]
        for j in reversed(range(tokens // chunk)):
            span = slice(j * chunk, (j + 1) * chunk)
            rounded = state.astype(BF16)
            k_stage[h, span] = (gk[h, span].astype(F32) + mm(vd[h, span], rounded, ABT)).astype(BF16)
            v_stage[h, span] = (gv[h, span].astype(F32) + mm(kd[h, span], rounded, AB)).astype(BF16)
            if j > 0:
                state = etot_ref[j, pl.ds(h, 1)] * state + lc[h, j]
        ready[2].start()
        ready[3].start()

    def wait(h):
        for copy in copies(h):
            copy.wait()

    store_gain = pltpu.make_async_copy(gg, gg_hbm, gain_sem.at[0])
    store_gain.start()
    loop(heads, first)
    loop(heads, one)
    loop(heads, wait)
    store_gain.wait()


def on_device(n, peers, queries, key_rows, value_rows, log_decay, norm_gain, grad_out):
    tokens, width = queries.shape
    heads = width // DH
    chunk = CHUNK if tokens % CHUNK == 0 else tokens
    chunks = tokens // chunk
    gain = norm_gain.reshape(heads, DH)
    anywhere = pl.BlockSpec(memory_space=pl.ANY)
    vmem = pl.BlockSpec(memory_space=pltpu.VMEM)
    rows = jax.ShapeDtypeStruct((tokens, width), BF16)
    states = jax.ShapeDtypeStruct((heads, chunks, DH, DH), BF16)
    per_head = lambda *shape, dtype=F32: pltpu.VMEM((heads, *shape), dtype)
    dma = pltpu.SemaphoreType.DMA
    led, chips = heads // GROUPS // 2, n // 2
    half = led * DH // chips
    parts = DH // half
    buf = lambda *shape: pltpu.VMEM((*shape, DH), F32)
    scan = [
        buf(led, DH + 8), buf(led, DH + 8), buf(led, DH + 8), buf(led, parts, half + 8),
        buf(chips, half + 8), buf(chips, half + 8), buf(led, parts, half + 8),
        buf(led, DH + 8), buf(led, DH + 8),
        dma((2, led)), dma((led, parts)), dma((chips,)), dma((chips,)), dma((led, parts)), dma((2, led)),
    ]
    by_head = lambda dtype: pltpu.VMEM((heads, tokens, DH), dtype)
    *held, grad_gain, state_grads = pl.pallas_call(
        functools.partial(main_kernel, n, peers, chunk),
        out_shape=(
            *[by_head(BF16)] * 6,
            pltpu.VMEM((heads, DH, DH), F32), pltpu.VMEM((chunks, heads, DH), F32),
            pltpu.VMEM((heads, DH), F32), pltpu.VMEM((heads, chunks, DH, DH), F32),
        ),
        in_specs=[anywhere] * 6,
        out_specs=(vmem,) * 10,
        scratch_shapes=[
            by_head(BF16), by_head(BF16), by_head(BF16), by_head(F32), pltpu.VMEM((heads, tokens), F32),
            per_head(chunks, DH, DH, dtype=BF16), buf(led, DH),
            pltpu.VMEM((tokens, DH), F32), pltpu.VMEM((tokens, DH), F32),
            pltpu.VMEM((chunks, 8, chunk), F32), pltpu.VMEM((chunks, peers, 8, chunk), F32),
            pltpu.VMEM((tokens, DH), F32), pltpu.VMEM((tokens, DH), F32), per_head(8, DH),
            *scan * (2 * GROUPS),
            pltpu.VMEM((heads, tokens), F32), pltpu.VMEM((heads, DH), F32),
            dma((4, heads)), dma((2, chunks, peers)), dma((2,)),
        ],
        compiler_params=pltpu.CompilerParams(
            collective_id=0, has_side_effects=True, vmem_limit_bytes=36 * 1024 * 1024
        ),
        name="forward_chain",
    )(queries, key_rows, value_rows, grad_out, log_decay, gain)
    grad_q, key_faded, value_faded, grad_v, grad_k, out, after, totals = held
    out, grad_q, grad_k, grad_v, grad_gain = pl.pallas_call(
        functools.partial(last_kernel, chunk),
        out_shape=(rows,) * 4 + (jax.ShapeDtypeStruct((heads, DH), F32),),
        in_specs=[vmem] * 10,
        out_specs=(anywhere,) * 5,
        scratch_shapes=[
            per_head(tokens, DH, dtype=BF16), per_head(tokens, DH, dtype=BF16), dma((4, heads)), dma((1,)),
        ],
        compiler_params=pltpu.CompilerParams(vmem_limit_bytes=10 * 1024 * 1024),
        name="last_terms",
    )(key_faded, value_faded, grad_q, grad_k, grad_v, out, after, totals, state_grads, grad_gain)
    return out, grad_q, grad_k, grad_v, grad_gain.reshape(width)


def solution(mesh):
    in_specs = (
        P("seq", "head"),
        P("seq", "head"),
        P("seq", "head"),
        P("head", "seq"),
        P("head"),
        P("seq", "head"),
    )
    out_specs = (P("seq", "head"), P("seq", "head"), P("seq", "head"), P("seq", "head"), P("head"))
    return jax.shard_map(
        functools.partial(on_device, mesh.shape["seq"], mesh.shape["head"]),
        mesh=mesh, in_specs=in_specs, out_specs=out_specs, check_vma=False,
    )
```

```python
import functools

import jax
import jax.numpy as jnp
from jax import lax
from jax.experimental import pallas as pl
from jax.experimental.pallas import tpu as pltpu
from jax.sharding import PartitionSpec as P

DH = 128
EPSILON = 1e-06
CHUNK = 256
GROUPS = 1
WIDE_GIVE = 8
WIDE_KEEP = 4
SPLIT_FORWARD = (8,)
SPLIT_BACKWARD = (8,)
F32 = jnp.float32
BF16 = jnp.bfloat16
MESH = pl.DeviceIdType.MESH
HIGHEST = lax.Precision.HIGHEST


def mm(left, right, dims):
    return lax.dot_general(left, right, (dims, ((), ())), preferred_element_type=F32)


AB = ((1,), (0,))
ABT = ((1,), (1,))
ATB = ((0,), (0,))


def chunk_cumsum(ld_ref, cum_ref, chunk):
    below = lax.broadcasted_iota(jnp.int32, (chunk, chunk), 0)
    right = lax.broadcasted_iota(jnp.int32, (chunk, chunk), 1)
    tri = (below <= right).astype(F32)
    for j in range(ld_ref.shape[1] // chunk):
        span = slice(j * chunk, (j + 1) * chunk)
        cum_ref[:, span] = lax.dot_general(
            ld_ref[:, span], tri, (AB, ((), ())), precision=HIGHEST, preferred_element_type=F32
        )


def cum_forms(cum_ref, h, j, chunk):
    row = cum_ref[pl.ds(h, 1), j * chunk : (j + 1) * chunk]
    column = jnp.broadcast_to(row, (DH, chunk)).T
    return row, column


def decay_of(row, column):
    chunk = row.shape[1]
    wide = jnp.concatenate([column] * (chunk // DH), axis=1)
    t = lax.broadcasted_iota(jnp.int32, (chunk, chunk), 0)
    s = lax.broadcasted_iota(jnp.int32, (chunk, chunk), 1)
    return jnp.where(t >= s, jnp.exp(wide - row), 0.0)


def remote(src, dst, send, recv, axis, target):
    return pltpu.make_async_remote_copy(
        src_ref=src, dst_ref=dst, send_sem=send, recv_sem=recv,
        device_id={axis: target}, device_id_type=MESH,
    )


def loop(count, body):
    lax.fori_loop(0, count, lambda i, c: (body(i), c)[1], 0)


def wide_loop(count, many, body):
    many = many if count % many == 0 else 1
    loop(count // many, lambda i: [body(many * i + p) for p in range(many)])


def group_loop(count, many, body):
    many = many if count % many == 0 else 1
    loop(count // many, lambda i: body([many * i + p for p in range(many)]))


class Scan:
    def __init__(self, n, reverse, base, bufs, decays=None):
        (
            self.lsend, self.lrecv, self.own, self.csend, self.arecv, self.asend, self.brecv,
            self.xsend, self.xrecv, self.lsem, self.asend_sem, self.arecv_sem,
            self.bsend_sem, self.brecv_sem, self.xsem,
        ) = bufs
        self.reverse = reverse
        self.base = base
        self.chips = n // 2
        self.led = self.lsend.shape[0]
        self.half = self.led * DH // self.chips
        self.parts = DH // self.half
        me = lax.axis_index("seq")
        self.core = lax.rem(me, 2)
        self.chip = me // 2
        self.partner = me + 1 - 2 * self.core
        self.am_first = self.core == (1 if reverse else 0)
        self.mine = self.chip // self.parts
        self.part = lax.rem(self.chip, self.parts)
        self.back = self.half + 1 if reverse else self.half
        self.cross = DH + 1 if reverse else DH
        self.decays = self if decays is None else decays
        self.deep = 4 if self.chips % 4 == 0 else self.chips
        wide = self.chips // self.deep
        distance = lambda d, size: min(d, size - d)
        offsets = [(dx, dz) for dx in range(wide) for dz in range(self.deep)][1:]
        self.order = sorted(offsets, key=lambda o: -distance(o[0], wide) - distance(o[1], self.deep))

    def led_head(self, j):
        return self.base + 2 * j + self.core

    def other_head(self, j):
        return self.base + 2 * j + 1 - self.core

    def turned(self, i):
        far = self.led // 2 + lax.rem(i, 2) * 2 * ((i + 1) // 2) - (i + 1) // 2
        return lax.rem(far + self.mine, self.led)

    def chip_at(self, dx, dz):
        x = lax.rem(self.chip // self.deep + dx, self.chips // self.deep)
        return x * self.deep + lax.rem(lax.rem(self.chip, self.deep) + dz, self.deep)

    def copy_l(self, j):
        return remote(self.lsend.at[j], self.lrecv.at[j], self.lsem.at[0, j], self.lsem.at[1, j], "seq", self.partner)

    def copy_a(self, j, b, chip):
        return remote(
            self.csend.at[j, b, pl.ds(0, self.half + 1)], self.arecv.at[chip, pl.ds(0, self.half + 1)], self.asend_sem.at[j, b], self.arecv_sem.at[chip],
            "seq", 2 * (self.parts * j + b) + self.core,
        )

    def copy_b(self, c, j, b):
        rows = pl.ds(0, self.back)
        return remote(
            self.asend.at[c, rows], self.brecv.at[j, b, rows], self.bsend_sem.at[c], self.brecv_sem.at[j, b],
            "seq", 2 * c + self.core,
        )

    def copy_x(self, j):
        rows = pl.ds(0, self.cross)
        return remote(self.xsend.at[j, rows], self.xrecv.at[j, rows], self.xsem.at[0, j], self.xsem.at[1, j], "seq", self.partner)

    def away(self, j, b):
        return self.parts * j + b != self.chip

    def give(self, j, state, extra):
        self.lsend[j, 0:DH] = state
        self.lsend[j, DH : DH + 8] = jnp.broadcast_to(extra, (8, DH))

    def keep(self, j, state, extra):
        self.own[j, 0:DH] = state
        self.own[j, DH : DH + 8] = jnp.broadcast_to(extra, (8, DH))
        self.copy_l(j).wait_recv()
        theirs = self.lrecv[j, 0:DH]
        first = jnp.where(self.am_first, state, theirs)
        second = jnp.where(self.am_first, theirs, state)
        mine, other = self.decays.own[j, DH : DH + 8], self.decays.lrecv[j, DH : DH + 8]
        decay_second = jnp.where(self.am_first, other, mine)[0:1]
        both = decay_second * first + second
        if self.reverse:
            tail = jnp.sum(self.own[j, DH : DH + 8] + self.lrecv[j, DH : DH + 8], axis=0, keepdims=True)
        else:
            tail = (mine * other)[0:1]
        for b in range(self.parts):
            self.csend[j, b, 0 : self.half] = both[b * self.half : (b + 1) * self.half]
            self.csend[j, b, self.half : self.half + 8] = jnp.broadcast_to(tail, (8, DH))
        for step in range(self.parts):
            b = lax.rem(self.part + self.parts // 2 + step, self.parts)

            @pl.when(self.away(j, b))
            def _():
                self.copy_a(j, b, self.chip).start()

            @pl.when(jnp.logical_not(self.away(j, b)))
            def _():
                self.arecv[self.chip] = self.csend[j, b]

    def combine(self):
        def arrive(c):
            @pl.when(c != self.chip)
            def _():
                self.copy_a(self.mine, self.part, c).wait_recv()

        if self.reverse:
            loop(self.chips, arrive)
            total = self.arecv[0, self.half : self.half + 1]
            for c in range(1, self.chips):
                total = total + self.arecv[c, self.half : self.half + 1]
            total = jnp.broadcast_to(total, (8, DH))

        def one(i, state):
            c = self.chips - 1 - i if self.reverse else i
            if not self.reverse:
                arrive(c)
            self.asend[c, 0 : self.half] = state
            if self.reverse:
                self.asend[c, self.half : self.half + 8] = total
            decay = self.decays.arecv[c, self.half : self.half + 1]
            return decay * state + self.arecv[c, 0 : self.half]

        lax.fori_loop(0, self.chips, one, jnp.zeros((self.half, DH), F32))
        for dx, dz in self.order:
            c = self.chip_at(dx, dz)
            self.copy_b(c, self.mine, self.part).start()
        self.brecv[self.mine, self.part, 0 : self.half] = self.asend[self.chip, 0 : self.half]
        if self.reverse:
            self.brecv[self.mine, self.part, self.half : self.half + 1] = self.asend[self.chip, self.half : self.half + 1]

    def take(self, j, state_ref):
        for b in range(self.parts):
            @pl.when(self.away(j, b))
            def _():
                self.copy_b(self.chip, j, b).wait_recv()

        base = jnp.concatenate([self.brecv[j, b, 0 : self.half] for b in range(self.parts)], axis=0)
        decay = jnp.where(self.am_first, self.decays.own[j, DH : DH + 8], self.decays.lrecv[j, DH : DH + 8])[0:1]
        held = jnp.where(self.am_first, self.own[j, 0:DH], self.lrecv[j, 0:DH])
        after = decay * base + held
        state_ref[...] = jnp.where(self.am_first, base, after)
        self.xsend[j, 0:DH] = jnp.where(self.am_first, after, base)
        if self.reverse:
            self.xsend[j, DH : DH + 1] = self.brecv[j, 0, self.half : self.half + 1]
        self.copy_x(j).start()

    def finish(self, j):
        self.copy_l(j).wait_send()
        self.copy_x(j).wait_send()
        for b in range(self.parts):
            @pl.when(self.away(j, b))
            def _():
                self.copy_a(j, b, self.chip).wait_send()

    def finish_chips(self):
        for dx, dz in self.order:
            self.copy_b(self.chip_at(dx, dz), self.mine, self.part).wait_send()


def main_kernel(
    n, peers, chunk,
    q_hbm, k_hbm, v_hbm, g_hbm, ld_hbm, gain_hbm,
    q, kd, vd, g, gk, obuf, r_out, etot_ref, gg_out, lc,
    k, v, qd, att, cum_ref, s_out, state_in, sq_acc, in_acc,
    stat_send, stat_recv, inv_b, cen_b, gain_acc, *rest,
):
    ld_ref, gain_ref, load_sem, stat_sem, small_sem = rest[-5:]
    bufs = [rest[15 * i : 15 * (i + 1)] for i in range(2 * GROUPS)]
    heads, tokens, _ = q.shape
    chunks = tokens // chunk
    me = lax.axis_index("seq")
    my_head = lax.axis_index("head")
    columns = heads * DH * peers

    def load(i, hbm, vmem, h):
        where = pl.ds(pl.multiple_of(h * DH, DH), DH)
        return pltpu.make_async_copy(hbm.at[:, where], vmem.at[h], load_sem.at[i, h])

    def load_kv(h):
        load(0, k_hbm, k, h).start()
        load(1, v_hbm, v, h).start()

    def load_q(h):
        load(2, q_hbm, q, h).start()

    def load_g(h):
        load(3, g_hbm, g, h).start()

    load_ld = pltpu.make_async_copy(ld_hbm, ld_ref, small_sem.at[0])
    load_gain = pltpu.make_async_copy(gain_hbm, gain_ref, small_sem.at[1])
    load_ld.start()
    load_gain.start()
    barrier = pltpu.get_barrier_semaphore()
    for off in range(1, n // 2):
        pl.semaphore_signal(barrier, inc=1, device_id={"seq": lax.rem(me + 2 * off, n)}, device_id_type=MESH)
    pl.semaphore_signal(barrier, inc=1, device_id={"seq": me + 1 - 2 * lax.rem(me, 2)}, device_id_type=MESH)
    for off in range(1, peers):
        pl.semaphore_signal(barrier, inc=1, device_id={"head": lax.rem(my_head + off, peers)}, device_id_type=MESH)


    each = heads // GROUPS
    forward = [Scan(n, False, i * each, bufs[i]) for i in range(GROUPS)]
    backward = [Scan(n, True, i * each, bufs[GROUPS + i], forward[i]) for i in range(GROUPS)]
    led = each // 2

    for scan in forward:
        loop(led, lambda j, scan=scan: load_kv(scan.other_head(j)))
        loop(led, lambda i, scan=scan: load_kv(scan.led_head(scan.turned(i))))
    load_ld.wait()
    load_gain.wait()
    chunk_cumsum(ld_ref, cum_ref, chunk)
    for j in range(chunks):
        end = (j + 1) * chunk
        etot_ref[j] = jnp.exp(jnp.broadcast_to(cum_ref[:, end - 1 : end], (heads, DH)))

    def total_of(h, j):
        return etot_ref[j, pl.ds(h, 1)]

    def local_state(h):
        load(0, k_hbm, k, h).wait()
        load(1, v_hbm, v, h).wait()
        state = decay = None
        for j in range(chunks):
            span = slice(j * chunk, (j + 1) * chunk)
            _, column = cum_forms(cum_ref, h, j, chunk)
            tail = jnp.exp(column[chunk - 1 : chunk, :] - column)
            faded = (k[h, span].astype(F32) * tail).astype(BF16)
            kd[h, span] = faded
            part = mm(faded, v[h, span], ATB)
            lc[h, j] = part
            total = total_of(h, j)
            state = part if j == 0 else total * state + part
            decay = total if j == 0 else decay * total
        return state, decay

    for i, scan in enumerate(forward):
        def give_forward(js, scan=scan):
            made = [local_state(scan.other_head(j)) for j in js]
            for j, pair in zip(js, made):
                scan.give(j, *pair)

        def keep_forward(steps, scan=scan):
            js = [scan.turned(i) for i in steps]
            made = [local_state(scan.led_head(j)) for j in js]
            for j, pair in zip(js, made):
                scan.keep(j, *pair)

        group_loop(led, WIDE_GIVE, give_forward)
        if i == 0:
            pl.semaphore_wait(barrier, n // 2 - 1 + 1 + peers - 1)
        loop(led, lambda j, scan=scan: scan.copy_l(j).start())
        group_loop(led, WIDE_KEEP, keep_forward)
    loop(heads, load_q)
    loop(heads, load_g)

    def intra(h):
        load(2, q_hbm, q, h).wait()
        for j in range(chunks):
            span = slice(j * chunk, (j + 1) * chunk)
            row, column = cum_forms(cum_ref, h, j, chunk)
            scores = mm(q[h, span], k[h, span], ABT)
            weights = (scores * decay_of(row, column)).astype(BF16)
            att[h, span] = mm(weights, v[h, span], AB)
            qd[h, span] = (q[h, span].astype(F32) * jnp.exp(column)).astype(BF16)
            tail = jnp.exp(column[chunk - 1 : chunk, :] - column)
            vd[h, span] = (v[h, span].astype(F32) * tail).astype(BF16)

    def between(splits, scans, body):
        edges = (0, *splits, heads)
        for i, (low, high) in enumerate(zip(edges, edges[1:])):
            wide_loop(high - low, 2, lambda h, low=low: body(h + low))
            if i < len(scans):
                scans[i].combine()

    between(SPLIT_FORWARD, forward, intra)

    sq_acc[...] = jnp.zeros_like(sq_acc)
    in_acc[...] = jnp.zeros_like(in_acc)

    gain_acc[...] = jnp.zeros_like(gain_acc)
    loop(heads, lambda h: load(3, g_hbm, g, h).wait())

    def spread(h, state):
        for j in range(chunks):
            s_out[h, j] = state.astype(BF16)
            if j < chunks - 1:
                state = total_of(h, j) * state + lc[h, j]

    def inter(j, pair):
        span = pl.ds(j * chunk if isinstance(j, int) else pl.multiple_of(j * chunk, chunk), chunk)
        square = inner = None
        for h in pair:
            whole = att[h, span] + mm(qd[h, span], s_out[h, j], AB)
            att[h, span] = whole
            scaled = g[h, span].astype(F32) * gain_ref[pl.ds(h, 1), :]
            square = whole * whole if square is None else square + whole * whole
            inner = scaled * whole if inner is None else inner + scaled * whole
        sq_acc[span] += square
        in_acc[span] += inner

    ones = jnp.ones((8, DH), F32)

    def row_sums(acc):
        return lax.dot_general(ones, acc, (ABT, ((), ())), precision=HIGHEST, preferred_element_type=F32)

    upper = lax.broadcasted_iota(jnp.int32, (8, chunk), 0) < 4

    def stat_copy(j, off, slot):
        return remote(
            stat_send.at[j], stat_recv.at[j, slot], stat_sem.at[0, j, off], stat_sem.at[1, j, off],
            "head", lax.rem(my_head + off, peers),
        )

    def send_stats(j):
        span = slice(j * chunk, (j + 1) * chunk)
        stat_send[j] = jnp.where(upper, row_sums(sq_acc[span]), row_sums(in_acc[span]))
        for off in range(1, peers):
            stat_copy(j, off, my_head).start()
        stat_recv[j, my_head] = stat_send[j]

    for i, scan in enumerate(forward):
        def take_forward(j, scan=scan):
            scan.take(j, state_in.at[j])
            spread(scan.led_head(j), state_in[j])

        def take_other_forward(j, scan=scan):
            scan.copy_x(j).wait_recv()
            spread(scan.other_head(j), scan.xrecv[j, 0:DH])

        everyone = [scan.base + h for h in range(each)]
        loop(led, take_forward)
        if i < GROUPS - 1:
            loop(led, take_other_forward)
            loop(chunks, lambda j, everyone=everyone: inter(j, everyone))
            continue
        inter(0, [scan.led_head(j) for j in range(led)])
        loop(led, take_other_forward)
        inter(0, [scan.other_head(j) for j in range(led)])
        send_stats(0)
        for j in range(1, chunks):
            inter(j, everyone)
            send_stats(j)

    def take_stats(j):
        span = slice(j * chunk, (j + 1) * chunk)
        for off in range(1, peers):
            stat_copy(j, off, lax.rem(my_head + peers - off, peers)).wait_recv()
        stats = stat_recv[j, 0]
        for i in range(1, peers):
            stats = stats + stat_recv[j, i]
        inverse = lax.rsqrt(stats[0:1] / columns + EPSILON)
        center = stats[4:5] * inverse / columns
        inv_b[span] = jnp.broadcast_to(inverse, (DH, chunk)).T
        cen_b[span] = jnp.broadcast_to(inverse * inverse * center, (DH, chunk)).T

    def normalize(j, h):
        span = slice(j * chunk, (j + 1) * chunk)
        gain = gain_ref[pl.ds(h, 1), :]
        whole = att[h, span]
        normed = whole * inv_b[span]
        obuf[h, span] = (normed * gain).astype(BF16)
        cotangent = g[h, span].astype(F32)
        product = cotangent * normed
        gain_acc[h] += jnp.sum(product.reshape(chunk // 8, 8, DH), axis=0)
        grad = (inv_b[span] * (cotangent * gain) - whole * cen_b[span]).astype(BF16)
        g[h, span] = grad
        return mm(qd[h, span], grad, ATB)

    def normalize_early(j, h):
        lc[h, j] = normalize(j, h)

    for j in range(chunks - 1):
        take_stats(j)
        wide_loop(heads, 8, functools.partial(normalize_early, j))
    take_stats(chunks - 1)

    def normalize_last(h):
        state = normalize(chunks - 1, h)
        lc[h, chunks - 1] = state
        for j in reversed(range(chunks - 1)):
            state = total_of(h, j) * state + lc[h, j]
        return state, gain_acc[h]

    for scan in backward:
        def give_backward(js, scan=scan):
            made = [normalize_last(scan.other_head(j)) for j in js]
            for j, pair in zip(js, made):
                scan.give(j, *pair)
                scan.copy_l(j).start()

        def keep_backward(steps, scan=scan):
            js = [scan.turned(i) for i in steps]
            made = [normalize_last(scan.led_head(j)) for j in js]
            for j, pair in zip(js, made):
                scan.keep(j, *pair)

        group_loop(led, WIDE_GIVE, give_backward)
        group_loop(led, WIDE_KEEP, keep_backward)

    def gradients(h):
        for j in range(chunks):
            span = slice(j * chunk, (j + 1) * chunk)
            row, column = cum_forms(cum_ref, h, j, chunk)
            decay = decay_of(row, column)
            queries, keys, values, grad = q[h, span], k[h, span], v[h, span], g[h, span]
            weights = (mm(queries, keys, ABT) * decay).astype(BF16)
            grad_weights = (mm(grad, values, ABT) * decay).astype(BF16)
            q[h, span] = (
                mm(grad_weights, keys, AB) + jnp.exp(column) * mm(grad, s_out[h, j], ABT)
            ).astype(BF16)
            gk[h, span] = mm(grad_weights, queries, ATB).astype(BF16)
            g[h, span] = mm(weights, grad, ATB).astype(BF16)

    between(SPLIT_BACKWARD, backward, gradients)

    for scan in backward:
        def take_led(j, scan=scan):
            h = scan.led_head(j)
            scan.take(j, r_out.at[h])
            gg_out[pl.ds(h, 1), :] = scan.xsend[j, DH : DH + 1]

        loop(led, take_led)

    for scan in backward:
        def take_other(j, scan=scan):
            h = scan.other_head(j)
            scan.copy_x(j).wait_recv()
            r_out[h] = scan.xrecv[j, 0:DH]
            gg_out[pl.ds(h, 1), :] = scan.xrecv[j, DH : DH + 1]

        loop(led, take_other)

    for scan in forward + backward:
        loop(led, scan.finish)
        scan.finish_chips()
    for j in range(chunks):
        for off in range(1, peers):
            stat_copy(j, off, my_head).wait_send()


def last_kernel(
    chunk, kd, vd, gq, gk, gv, out, after, etot_ref, lc, gg,
    out_hbm, gq_hbm, gk_hbm, gv_hbm, gg_hbm, k_stage, v_stage, store_sem, gain_sem,
):
    heads, tokens, _ = kd.shape

    def store(i, vmem, hbm, h):
        where = pl.ds(pl.multiple_of(h * DH, DH), DH)
        return pltpu.make_async_copy(vmem.at[h], hbm.at[:, where], store_sem.at[i, h])

    def copies(h):
        return (
            store(0, out, out_hbm, h), store(1, gq, gq_hbm, h),
            store(2, k_stage, gk_hbm, h), store(3, v_stage, gv_hbm, h),
        )

    def first(h):
        ready = copies(h)
        ready[0].start()
        ready[1].start()

    def one(h):
        ready = copies(h)
        state = after[h]
        for j in reversed(range(tokens // chunk)):
            span = slice(j * chunk, (j + 1) * chunk)
            rounded = state.astype(BF16)
            k_stage[h, span] = (gk[h, span].astype(F32) + mm(vd[h, span], rounded, ABT)).astype(BF16)
            v_stage[h, span] = (gv[h, span].astype(F32) + mm(kd[h, span], rounded, AB)).astype(BF16)
            if j > 0:
                state = etot_ref[j, pl.ds(h, 1)] * state + lc[h, j]
        ready[2].start()
        ready[3].start()

    def wait(h):
        for copy in copies(h):
            copy.wait()

    store_gain = pltpu.make_async_copy(gg, gg_hbm, gain_sem.at[0])
    store_gain.start()
    loop(heads, first)
    loop(heads, one)
    loop(heads, wait)
    store_gain.wait()


def on_device(n, peers, queries, key_rows, value_rows, log_decay, norm_gain, grad_out):
    tokens, width = queries.shape
    heads = width // DH
    chunk = CHUNK if tokens % CHUNK == 0 else tokens
    chunks = tokens // chunk
    gain = norm_gain.reshape(heads, DH)
    anywhere = pl.BlockSpec(memory_space=pl.ANY)
    vmem = pl.BlockSpec(memory_space=pltpu.VMEM)
    rows = jax.ShapeDtypeStruct((tokens, width), BF16)
    states = jax.ShapeDtypeStruct((heads, chunks, DH, DH), BF16)
    per_head = lambda *shape, dtype=F32: pltpu.VMEM((heads, *shape), dtype)
    dma = pltpu.SemaphoreType.DMA
    led, chips = heads // GROUPS // 2, n // 2
    half = led * DH // chips
    parts = DH // half
    buf = lambda *shape: pltpu.VMEM((*shape, DH), F32)
    scan = [
        buf(led, DH + 8), buf(led, DH + 8), buf(led, DH + 8), buf(led, parts, half + 8),
        buf(chips, half + 8), buf(chips, half + 8), buf(led, parts, half + 8),
        buf(led, DH + 8), buf(led, DH + 8),
        dma((2, led)), dma((led, parts)), dma((chips,)), dma((chips,)), dma((led, parts)), dma((2, led)),
    ]
    by_head = lambda dtype: pltpu.VMEM((heads, tokens, DH), dtype)
    *held, grad_gain, state_grads = pl.pallas_call(
        functools.partial(main_kernel, n, peers, chunk),
        out_shape=(
            *[by_head(BF16)] * 6,
            pltpu.VMEM((heads, DH, DH), F32), pltpu.VMEM((chunks, heads, DH), F32),
            pltpu.VMEM((heads, DH), F32), pltpu.VMEM((heads, chunks, DH, DH), F32),
        ),
        in_specs=[anywhere] * 6,
        out_specs=(vmem,) * 10,
        scratch_shapes=[
            by_head(BF16), by_head(BF16), by_head(BF16), by_head(F32), pltpu.VMEM((heads, tokens), F32),
            per_head(chunks, DH, DH, dtype=BF16), buf(led, DH),
            pltpu.VMEM((tokens, DH), F32), pltpu.VMEM((tokens, DH), F32),
            pltpu.VMEM((chunks, 8, chunk), F32), pltpu.VMEM((chunks, peers, 8, chunk), F32),
            pltpu.VMEM((tokens, DH), F32), pltpu.VMEM((tokens, DH), F32), per_head(8, DH),
            *scan * (2 * GROUPS),
            pltpu.VMEM((heads, tokens), F32), pltpu.VMEM((heads, DH), F32),
            dma((4, heads)), dma((2, chunks, peers)), dma((2,)),
        ],
        compiler_params=pltpu.CompilerParams(
            collective_id=0, has_side_effects=True, vmem_limit_bytes=36 * 1024 * 1024
        ),
        name="forward_chain",
    )(queries, key_rows, value_rows, grad_out, log_decay, gain)
    grad_q, key_faded, value_faded, grad_v, grad_k, out, after, totals = held
    out, grad_q, grad_k, grad_v, grad_gain = pl.pallas_call(
        functools.partial(last_kernel, chunk),
        out_shape=(rows,) * 4 + (jax.ShapeDtypeStruct((heads, DH), F32),),
        in_specs=[vmem] * 10,
        out_specs=(anywhere,) * 5,
        scratch_shapes=[
            per_head(tokens, DH, dtype=BF16), per_head(tokens, DH, dtype=BF16), dma((4, heads)), dma((1,)),
        ],
        compiler_params=pltpu.CompilerParams(vmem_limit_bytes=10 * 1024 * 1024),
        name="last_terms",
    )(key_faded, value_faded, grad_q, grad_k, grad_v, out, after, totals, state_grads, grad_gain)
    return out, grad_q, grad_k, grad_v, grad_gain.reshape(width)


def solution(mesh):
    in_specs = (
        P("seq", "head"),
        P("seq", "head"),
        P("seq", "head"),
        P("head", "seq"),
        P("head"),
        P("seq", "head"),
    )
    out_specs = (P("seq", "head"), P("seq", "head"), P("seq", "head"), P("seq", "head"), P("head"))
    return jax.shard_map(
        functools.partial(on_device, mesh.shape["seq"], mesh.shape["head"]),
        mesh=mesh, in_specs=in_specs, out_specs=out_specs, check_vma=False,
    )
```

```python
import functools

import jax
import jax.numpy as jnp
from jax import lax
from jax.experimental import pallas as pl
from jax.experimental.pallas import tpu as pltpu
from jax.sharding import PartitionSpec as P

DH = 128
EPSILON = 1e-06
CHUNK = 256
GROUPS = 1
WIDE_GIVE = 8
WIDE_KEEP = 4
SPLIT_FORWARD = (8,)
SPLIT_BACKWARD = (8,)
F32 = jnp.float32
BF16 = jnp.bfloat16
MESH = pl.DeviceIdType.MESH
HIGHEST = lax.Precision.HIGHEST


def mm(left, right, dims):
    return lax.dot_general(left, right, (dims, ((), ())), preferred_element_type=F32)


AB = ((1,), (0,))
ABT = ((1,), (1,))
ATB = ((0,), (0,))


def chunk_cumsum(ld_ref, cum_ref, chunk):
    below = lax.broadcasted_iota(jnp.int32, (chunk, chunk), 0)
    right = lax.broadcasted_iota(jnp.int32, (chunk, chunk), 1)
    tri = (below <= right).astype(F32)
    for j in range(ld_ref.shape[1] // chunk):
        span = slice(j * chunk, (j + 1) * chunk)
        cum_ref[:, span] = lax.dot_general(
            ld_ref[:, span], tri, (AB, ((), ())), precision=HIGHEST, preferred_element_type=F32
        )


def cum_forms(cum_ref, h, j, chunk):
    row = cum_ref[pl.ds(h, 1), j * chunk : (j + 1) * chunk]
    column = jnp.broadcast_to(row, (DH, chunk)).T
    return row, column


def decay_of(row, column):
    chunk = row.shape[1]
    wide = jnp.concatenate([column] * (chunk // DH), axis=1)
    t = lax.broadcasted_iota(jnp.int32, (chunk, chunk), 0)
    s = lax.broadcasted_iota(jnp.int32, (chunk, chunk), 1)
    return jnp.where(t >= s, jnp.exp(wide - row), 0.0)


def remote(src, dst, send, recv, axis, target):
    return pltpu.make_async_remote_copy(
        src_ref=src, dst_ref=dst, send_sem=send, recv_sem=recv,
        device_id={axis: target}, device_id_type=MESH,
    )


def loop(count, body):
    lax.fori_loop(0, count, lambda i, c: (body(i), c)[1], 0)


def wide_loop(count, many, body):
    many = many if count % many == 0 else 1
    loop(count // many, lambda i: [body(many * i + p) for p in range(many)])


def group_loop(count, many, body):
    many = many if count % many == 0 else 1
    loop(count // many, lambda i: body([many * i + p for p in range(many)]))


class Scan:
    def __init__(self, n, reverse, base, bufs, decays=None):
        (
            self.lsend, self.lrecv, self.own, self.csend, self.arecv, self.asend, self.brecv,
            self.xsend, self.xrecv, self.lsem, self.asend_sem, self.arecv_sem,
            self.bsend_sem, self.brecv_sem, self.xsem,
        ) = bufs
        self.reverse = reverse
        self.base = base
        self.chips = n // 2
        self.led = self.lsend.shape[0]
        self.half = self.led * DH // self.chips
        self.parts = DH // self.half
        me = lax.axis_index("seq")
        self.core = lax.rem(me, 2)
        self.chip = me // 2
        self.partner = me + 1 - 2 * self.core
        self.am_first = self.core == (1 if reverse else 0)
        self.mine = self.chip // self.parts
        self.part = lax.rem(self.chip, self.parts)
        self.back = self.half + 1 if reverse else self.half
        self.cross = DH + 1 if reverse else DH
        self.decays = self if decays is None else decays
        self.deep = 4 if self.chips % 4 == 0 else self.chips
        wide = self.chips // self.deep
        distance = lambda d, size: min(d, size - d)
        offsets = [(dx, dz) for dx in range(wide) for dz in range(self.deep)][1:]
        self.order = sorted(offsets, key=lambda o: -distance(o[0], wide) - distance(o[1], self.deep))

    def led_head(self, j):
        return self.base + 2 * j + self.core

    def other_head(self, j):
        return self.base + 2 * j + 1 - self.core

    def turned(self, i):
        far = self.led // 2 + lax.rem(i, 2) * 2 * ((i + 1) // 2) - (i + 1) // 2
        return lax.rem(far + self.mine, self.led)

    def chip_at(self, dx, dz):
        x = lax.rem(self.chip // self.deep + dx, self.chips // self.deep)
        return x * self.deep + lax.rem(lax.rem(self.chip, self.deep) + dz, self.deep)

    def copy_l(self, j):
        return remote(self.lsend.at[j], self.lrecv.at[j], self.lsem.at[0, j], self.lsem.at[1, j], "seq", self.partner)

    def copy_a(self, j, b, chip):
        return remote(
            self.csend.at[j, b, pl.ds(0, self.half + 1)], self.arecv.at[chip, pl.ds(0, self.half + 1)], self.asend_sem.at[j, b], self.arecv_sem.at[chip],
            "seq", 2 * (self.parts * j + b) + self.core,
        )

    def copy_b(self, c, j, b):
        rows = pl.ds(0, self.back)
        return remote(
            self.asend.at[c, rows], self.brecv.at[j, b, rows], self.bsend_sem.at[c], self.brecv_sem.at[j, b],
            "seq", 2 * c + self.core,
        )

    def copy_x(self, j):
        rows = pl.ds(0, self.cross)
        return remote(self.xsend.at[j, rows], self.xrecv.at[j, rows], self.xsem.at[0, j], self.xsem.at[1, j], "seq", self.partner)

    def away(self, j, b):
        return self.parts * j + b != self.chip

    def give(self, j, state, extra):
        self.lsend[j, 0:DH] = state
        self.lsend[j, DH : DH + 8] = jnp.broadcast_to(extra, (8, DH))

    def keep(self, j, state, extra):
        self.own[j, 0:DH] = state
        self.own[j, DH : DH + 8] = jnp.broadcast_to(extra, (8, DH))
        self.copy_l(j).wait_recv()
        theirs = self.lrecv[j, 0:DH]
        first = jnp.where(self.am_first, state, theirs)
        second = jnp.where(self.am_first, theirs, state)
        mine, other = self.decays.own[j, DH : DH + 8], self.decays.lrecv[j, DH : DH + 8]
        decay_second = jnp.where(self.am_first, other, mine)[0:1]
        both = decay_second * first + second
        if self.reverse:
            tail = jnp.sum(self.own[j, DH : DH + 8] + self.lrecv[j, DH : DH + 8], axis=0, keepdims=True)
        else:
            tail = (mine * other)[0:1]
        for b in range(self.parts):
            self.csend[j, b, 0 : self.half] = both[b * self.half : (b + 1) * self.half]
            self.csend[j, b, self.half : self.half + 8] = jnp.broadcast_to(tail, (8, DH))
        for step in range(self.parts):
            b = lax.rem(self.part + self.parts // 2 + step, self.parts)

            @pl.when(self.away(j, b))
            def _():
                self.copy_a(j, b, self.chip).start()

            @pl.when(jnp.logical_not(self.away(j, b)))
            def _():
                self.arecv[self.chip] = self.csend[j, b]

    def combine(self):
        def arrive(c):
            @pl.when(c != self.chip)
            def _():
                self.copy_a(self.mine, self.part, c).wait_recv()

        if self.reverse:
            loop(self.chips, arrive)
            total = self.arecv[0, self.half : self.half + 1]
            for c in range(1, self.chips):
                total = total + self.arecv[c, self.half : self.half + 1]
            total = jnp.broadcast_to(total, (8, DH))

        def one(i, state):
            c = self.chips - 1 - i if self.reverse else i
            if not self.reverse:
                arrive(c)
            self.asend[c, 0 : self.half] = state
            if self.reverse:
                self.asend[c, self.half : self.half + 8] = total
            decay = self.decays.arecv[c, self.half : self.half + 1]
            return decay * state + self.arecv[c, 0 : self.half]

        lax.fori_loop(0, self.chips, one, jnp.zeros((self.half, DH), F32))
        for dx, dz in self.order:
            c = self.chip_at(dx, dz)
            self.copy_b(c, self.mine, self.part).start()
        self.brecv[self.mine, self.part, 0 : self.half] = self.asend[self.chip, 0 : self.half]
        if self.reverse:
            self.brecv[self.mine, self.part, self.half : self.half + 1] = self.asend[self.chip, self.half : self.half + 1]

    def take(self, j, state_ref):
        for b in range(self.parts):
            @pl.when(self.away(j, b))
            def _():
                self.copy_b(self.chip, j, b).wait_recv()

        base = jnp.concatenate([self.brecv[j, b, 0 : self.half] for b in range(self.parts)], axis=0)
        decay = jnp.where(self.am_first, self.decays.own[j, DH : DH + 8], self.decays.lrecv[j, DH : DH + 8])[0:1]
        held = jnp.where(self.am_first, self.own[j, 0:DH], self.lrecv[j, 0:DH])
        after = decay * base + held
        state_ref[...] = jnp.where(self.am_first, base, after)
        self.xsend[j, 0:DH] = jnp.where(self.am_first, after, base)
        if self.reverse:
            self.xsend[j, DH : DH + 1] = self.brecv[j, 0, self.half : self.half + 1]
        self.copy_x(j).start()

    def finish(self, j):
        self.copy_l(j).wait_send()
        self.copy_x(j).wait_send()
        for b in range(self.parts):
            @pl.when(self.away(j, b))
            def _():
                self.copy_a(j, b, self.chip).wait_send()

    def finish_chips(self):
        for dx, dz in self.order:
            self.copy_b(self.chip_at(dx, dz), self.mine, self.part).wait_send()


def main_kernel(
    n, peers, chunk,
    q_hbm, k_hbm, v_hbm, g_hbm, ld_hbm, gain_hbm,
    q, kd, vd, g, gk, obuf, r_out, etot_ref, gg_out, lc,
    k, v, qd, att, cum_ref, s_out, state_in, sq_acc, in_acc,
    stat_send, stat_recv, inv_b, cen_b, gain_acc, *rest,
):
    ld_ref, gain_ref, load_sem, stat_sem, small_sem = rest[-5:]
    bufs = [rest[15 * i : 15 * (i + 1)] for i in range(2 * GROUPS)]
    heads, tokens, _ = q.shape
    chunks = tokens // chunk
    me = lax.axis_index("seq")
    my_head = lax.axis_index("head")
    columns = heads * DH * peers

    def load(i, hbm, vmem, h):
        where = pl.ds(pl.multiple_of(h * DH, DH), DH)
        return pltpu.make_async_copy(hbm.at[:, where], vmem.at[h], load_sem.at[i, h])

    def load_kv(h):
        load(0, k_hbm, k, h).start()
        load(1, v_hbm, v, h).start()

    def load_q(h):
        load(2, q_hbm, q, h).start()

    def load_g(h):
        load(3, g_hbm, g, h).start()

    load_ld = pltpu.make_async_copy(ld_hbm, ld_ref, small_sem.at[0])
    load_gain = pltpu.make_async_copy(gain_hbm, gain_ref, small_sem.at[1])
    load_ld.start()
    load_gain.start()
    barrier = pltpu.get_barrier_semaphore()
    for off in range(1, n // 2):
        pl.semaphore_signal(barrier, inc=1, device_id={"seq": lax.rem(me + 2 * off, n)}, device_id_type=MESH)
    pl.semaphore_signal(barrier, inc=1, device_id={"seq": me + 1 - 2 * lax.rem(me, 2)}, device_id_type=MESH)
    for off in range(1, peers):
        pl.semaphore_signal(barrier, inc=1, device_id={"head": lax.rem(my_head + off, peers)}, device_id_type=MESH)


    each = heads // GROUPS
    forward = [Scan(n, False, i * each, bufs[i]) for i in range(GROUPS)]
    backward = [Scan(n, True, i * each, bufs[GROUPS + i], forward[i]) for i in range(GROUPS)]
    led = each // 2

    for scan in forward:
        loop(led, lambda j, scan=scan: load_kv(scan.other_head(j)))
        loop(led, lambda i, scan=scan: load_kv(scan.led_head(scan.turned(i))))
    load_ld.wait()
    load_gain.wait()
    chunk_cumsum(ld_ref, cum_ref, chunk)
    for j in range(chunks):
        end = (j + 1) * chunk
        etot_ref[j] = jnp.exp(jnp.broadcast_to(cum_ref[:, end - 1 : end], (heads, DH)))

    def total_of(h, j):
        return etot_ref[j, pl.ds(h, 1)]

    def local_state(h):
        load(0, k_hbm, k, h).wait()
        load(1, v_hbm, v, h).wait()
        state = decay = None
        for j in range(chunks):
            span = slice(j * chunk, (j + 1) * chunk)
            _, column = cum_forms(cum_ref, h, j, chunk)
            tail = jnp.exp(column[chunk - 1 : chunk, :] - column)
            faded = (k[h, span].astype(F32) * tail).astype(BF16)
            kd[h, span] = faded
            part = mm(faded, v[h, span], ATB)
            lc[h, j] = part
            total = total_of(h, j)
            state = part if j == 0 else total * state + part
            decay = total if j == 0 else decay * total
        return state, decay

    for i, scan in enumerate(forward):
        def give_forward(js, scan=scan):
            made = [local_state(scan.other_head(j)) for j in js]
            for j, pair in zip(js, made):
                scan.give(j, *pair)

        def keep_forward(steps, scan=scan):
            js = [scan.turned(i) for i in steps]
            made = [local_state(scan.led_head(j)) for j in js]
            for j, pair in zip(js, made):
                scan.keep(j, *pair)

        group_loop(led, WIDE_GIVE, give_forward)
        if i == 0:
            pl.semaphore_wait(barrier, n // 2 - 1 + 1 + peers - 1)
        loop(led, lambda j, scan=scan: scan.copy_l(j).start())
        group_loop(led, WIDE_KEEP, keep_forward)
    loop(heads, load_q)
    loop(heads, load_g)

    def intra(h):
        load(2, q_hbm, q, h).wait()
        for j in range(chunks):
            span = slice(j * chunk, (j + 1) * chunk)
            row, column = cum_forms(cum_ref, h, j, chunk)
            scores = mm(q[h, span], k[h, span], ABT)
            weights = (scores * decay_of(row, column)).astype(BF16)
            att[h, span] = mm(weights, v[h, span], AB)
            qd[h, span] = (q[h, span].astype(F32) * jnp.exp(column)).astype(BF16)
            tail = jnp.exp(column[chunk - 1 : chunk, :] - column)
            vd[h, span] = (v[h, span].astype(F32) * tail).astype(BF16)

    def between(splits, scans, body):
        edges = (0, *splits, heads)
        for i, (low, high) in enumerate(zip(edges, edges[1:])):
            wide_loop(high - low, 2, lambda h, low=low: body(h + low))
            if i < len(scans):
                scans[i].combine()

    between(SPLIT_FORWARD, forward, intra)

    sq_acc[...] = jnp.zeros_like(sq_acc)
    in_acc[...] = jnp.zeros_like(in_acc)

    gain_acc[...] = jnp.zeros_like(gain_acc)
    loop(heads, lambda h: load(3, g_hbm, g, h).wait())

    def spread(h, state):
        for j in range(chunks):
            s_out[h, j] = state.astype(BF16)
            if j < chunks - 1:
                state = total_of(h, j) * state + lc[h, j]

    def inter(j, pair):
        span = pl.ds(j * chunk if isinstance(j, int) else pl.multiple_of(j * chunk, chunk), chunk)
        square = inner = None
        for h in pair:
            whole = att[h, span] + mm(qd[h, span], s_out[h, j], AB)
            att[h, span] = whole
            scaled = g[h, span].astype(F32) * gain_ref[pl.ds(h, 1), :]
            square = whole * whole if square is None else square + whole * whole
            inner = scaled * whole if inner is None else inner + scaled * whole
        sq_acc[span] += square
        in_acc[span] += inner

    ones = jnp.ones((8, DH), F32)

    def row_sums(acc):
        return lax.dot_general(ones, acc, (ABT, ((), ())), precision=HIGHEST, preferred_element_type=F32)

    upper = lax.broadcasted_iota(jnp.int32, (8, chunk), 0) < 4

    def stat_copy(j, off, slot):
        return remote(
            stat_send.at[j], stat_recv.at[j, slot], stat_sem.at[0, j, off], stat_sem.at[1, j, off],
            "head", lax.rem(my_head + off, peers),
        )

    def send_stats(j):
        span = slice(j * chunk, (j + 1) * chunk)
        stat_send[j] = jnp.where(upper, row_sums(sq_acc[span]), row_sums(in_acc[span]))
        for off in range(1, peers):
            stat_copy(j, off, my_head).start()
        stat_recv[j, my_head] = stat_send[j]

    for i, scan in enumerate(forward):
        def take_forward(j, scan=scan):
            scan.take(j, state_in.at[j])
            spread(scan.led_head(j), state_in[j])

        def take_other_forward(j, scan=scan):
            scan.copy_x(j).wait_recv()
            spread(scan.other_head(j), scan.xrecv[j, 0:DH])

        everyone = [scan.base + h for h in range(each)]
        loop(led, take_forward)
        if i < GROUPS - 1:
            loop(led, take_other_forward)
            loop(chunks, lambda j, everyone=everyone: inter(j, everyone))
            continue
        inter(0, [scan.led_head(j) for j in range(led)])
        loop(led, take_other_forward)
        inter(0, [scan.other_head(j) for j in range(led)])
        send_stats(0)
        for j in range(1, chunks):
            inter(j, everyone)
            send_stats(j)

    def take_stats(j):
        span = slice(j * chunk, (j + 1) * chunk)
        for off in range(1, peers):
            stat_copy(j, off, lax.rem(my_head + peers - off, peers)).wait_recv()
        stats = stat_recv[j, 0]
        for i in range(1, peers):
            stats = stats + stat_recv[j, i]
        inverse = lax.rsqrt(stats[0:1] / columns + EPSILON)
        center = stats[4:5] * inverse / columns
        inv_b[span] = jnp.broadcast_to(inverse, (DH, chunk)).T
        cen_b[span] = jnp.broadcast_to(inverse * inverse * center, (DH, chunk)).T

    def normalize(j, h):
        span = slice(j * chunk, (j + 1) * chunk)
        gain = gain_ref[pl.ds(h, 1), :]
        whole = att[h, span]
        normed = whole * inv_b[span]
        obuf[h, span] = (normed * gain).astype(BF16)
        cotangent = g[h, span].astype(F32)
        product = cotangent * normed
        gain_acc[h] += jnp.sum(product.reshape(chunk // 8, 8, DH), axis=0)
        grad = (inv_b[span] * (cotangent * gain) - whole * cen_b[span]).astype(BF16)
        g[h, span] = grad
        return mm(qd[h, span], grad, ATB)

    def normalize_early(j, h):
        lc[h, j] = normalize(j, h)

    for j in range(chunks - 1):
        take_stats(j)
        wide_loop(heads, 8, functools.partial(normalize_early, j))
    take_stats(chunks - 1)

    def normalize_last(h):
        state = normalize(chunks - 1, h)
        lc[h, chunks - 1] = state
        for j in reversed(range(chunks - 1)):
            state = total_of(h, j) * state + lc[h, j]
        return state, gain_acc[h]

    for scan in backward:
        def give_backward(js, scan=scan):
            made = [normalize_last(scan.other_head(j)) for j in js]
            for j, pair in zip(js, made):
                scan.give(j, *pair)
                scan.copy_l(j).start()

        def keep_backward(steps, scan=scan):
            js = [scan.turned(i) for i in steps]
            made = [normalize_last(scan.led_head(j)) for j in js]
            for j, pair in zip(js, made):
                scan.keep(j, *pair)

        group_loop(led, WIDE_GIVE, give_backward)
        group_loop(led, WIDE_KEEP, keep_backward)

    def gradients(h):
        for j in range(chunks):
            span = slice(j * chunk, (j + 1) * chunk)
            row, column = cum_forms(cum_ref, h, j, chunk)
            decay = decay_of(row, column)
            queries, keys, values, grad = q[h, span], k[h, span], v[h, span], g[h, span]
            weights = (mm(queries, keys, ABT) * decay).astype(BF16)
            grad_weights = (mm(grad, values, ABT) * decay).astype(BF16)
            q[h, span] = (
                mm(grad_weights, keys, AB) + jnp.exp(column) * mm(grad, s_out[h, j], ABT)
            ).astype(BF16)
            gk[h, span] = mm(grad_weights, queries, ATB).astype(BF16)
            g[h, span] = mm(weights, grad, ATB).astype(BF16)

    between(SPLIT_BACKWARD, backward, gradients)

    for scan in backward:
        def take_led(j, scan=scan):
            h = scan.led_head(j)
            scan.take(j, r_out.at[h])
            gg_out[pl.ds(h, 1), :] = scan.xsend[j, DH : DH + 1]

        loop(led, take_led)

    for scan in backward:
        def take_other(j, scan=scan):
            h = scan.other_head(j)
            scan.copy_x(j).wait_recv()
            r_out[h] = scan.xrecv[j, 0:DH]
            gg_out[pl.ds(h, 1), :] = scan.xrecv[j, DH : DH + 1]

        loop(led, take_other)

    for scan in forward + backward:
        loop(led, scan.finish)
        scan.finish_chips()
    for j in range(chunks):
        for off in range(1, peers):
            stat_copy(j, off, my_head).wait_send()


def last_kernel(
    chunk, kd, vd, gq, gk, gv, out, after, etot_ref, lc, gg,
    out_hbm, gq_hbm, gk_hbm, gv_hbm, gg_hbm, k_stage, v_stage, store_sem, gain_sem,
):
    heads, tokens, _ = kd.shape

    def store(i, vmem, hbm, h):
        where = pl.ds(pl.multiple_of(h * DH, DH), DH)
        return pltpu.make_async_copy(vmem.at[h], hbm.at[:, where], store_sem.at[i, h])

    def copies(h):
        return (
            store(0, out, out_hbm, h), store(1, gq, gq_hbm, h),
            store(2, k_stage, gk_hbm, h), store(3, v_stage, gv_hbm, h),
        )

    def first(h):
        ready = copies(h)
        ready[0].start()
        ready[1].start()

    def one(h):
        ready = copies(h)
        state = after[h]
        for j in reversed(range(tokens // chunk)):
            span = slice(j * chunk, (j + 1) * chunk)
            rounded = state.astype(BF16)
            k_stage[h, span] = (gk[h, span].astype(F32) + mm(vd[h, span], rounded, ABT)).astype(BF16)
            v_stage[h, span] = (gv[h, span].astype(F32) + mm(kd[h, span], rounded, AB)).astype(BF16)
            if j > 0:
                state = etot_ref[j, pl.ds(h, 1)] * state + lc[h, j]
        ready[2].start()
        ready[3].start()

    def wait(h):
        for copy in copies(h):
            copy.wait()

    store_gain = pltpu.make_async_copy(gg, gg_hbm, gain_sem.at[0])
    store_gain.start()
    loop(heads, first)
    wide_loop(heads, 2, one)
    loop(heads, wait)
    store_gain.wait()


def on_device(n, peers, queries, key_rows, value_rows, log_decay, norm_gain, grad_out):
    tokens, width = queries.shape
    heads = width // DH
    chunk = CHUNK if tokens % CHUNK == 0 else tokens
    chunks = tokens // chunk
    gain = norm_gain.reshape(heads, DH)
    anywhere = pl.BlockSpec(memory_space=pl.ANY)
    vmem = pl.BlockSpec(memory_space=pltpu.VMEM)
    rows = jax.ShapeDtypeStruct((tokens, width), BF16)
    states = jax.ShapeDtypeStruct((heads, chunks, DH, DH), BF16)
    per_head = lambda *shape, dtype=F32: pltpu.VMEM((heads, *shape), dtype)
    dma = pltpu.SemaphoreType.DMA
    led, chips = heads // GROUPS // 2, n // 2
    half = led * DH // chips
    parts = DH // half
    buf = lambda *shape: pltpu.VMEM((*shape, DH), F32)
    scan = [
        buf(led, DH + 8), buf(led, DH + 8), buf(led, DH + 8), buf(led, parts, half + 8),
        buf(chips, half + 8), buf(chips, half + 8), buf(led, parts, half + 8),
        buf(led, DH + 8), buf(led, DH + 8),
        dma((2, led)), dma((led, parts)), dma((chips,)), dma((chips,)), dma((led, parts)), dma((2, led)),
    ]
    by_head = lambda dtype: pltpu.VMEM((heads, tokens, DH), dtype)
    *held, grad_gain, state_grads = pl.pallas_call(
        functools.partial(main_kernel, n, peers, chunk),
        out_shape=(
            *[by_head(BF16)] * 6,
            pltpu.VMEM((heads, DH, DH), F32), pltpu.VMEM((chunks, heads, DH), F32),
            pltpu.VMEM((heads, DH), F32), pltpu.VMEM((heads, chunks, DH, DH), F32),
        ),
        in_specs=[anywhere] * 6,
        out_specs=(vmem,) * 10,
        scratch_shapes=[
            by_head(BF16), by_head(BF16), by_head(BF16), by_head(F32), pltpu.VMEM((heads, tokens), F32),
            per_head(chunks, DH, DH, dtype=BF16), buf(led, DH),
            pltpu.VMEM((tokens, DH), F32), pltpu.VMEM((tokens, DH), F32),
            pltpu.VMEM((chunks, 8, chunk), F32), pltpu.VMEM((chunks, peers, 8, chunk), F32),
            pltpu.VMEM((tokens, DH), F32), pltpu.VMEM((tokens, DH), F32), per_head(8, DH),
            *scan * (2 * GROUPS),
            pltpu.VMEM((heads, tokens), F32), pltpu.VMEM((heads, DH), F32),
            dma((4, heads)), dma((2, chunks, peers)), dma((2,)),
        ],
        compiler_params=pltpu.CompilerParams(
            collective_id=0, has_side_effects=True, vmem_limit_bytes=36 * 1024 * 1024
        ),
        name="forward_chain",
    )(queries, key_rows, value_rows, grad_out, log_decay, gain)
    grad_q, key_faded, value_faded, grad_v, grad_k, out, after, totals = held
    out, grad_q, grad_k, grad_v, grad_gain = pl.pallas_call(
        functools.partial(last_kernel, chunk),
        out_shape=(rows,) * 4 + (jax.ShapeDtypeStruct((heads, DH), F32),),
        in_specs=[vmem] * 10,
        out_specs=(anywhere,) * 5,
        scratch_shapes=[
            per_head(tokens, DH, dtype=BF16), per_head(tokens, DH, dtype=BF16), dma((4, heads)), dma((1,)),
        ],
        compiler_params=pltpu.CompilerParams(vmem_limit_bytes=10 * 1024 * 1024),
        name="last_terms",
    )(key_faded, value_faded, grad_q, grad_k, grad_v, out, after, totals, state_grads, grad_gain)
    return out, grad_q, grad_k, grad_v, grad_gain.reshape(width)


def solution(mesh):
    in_specs = (
        P("seq", "head"),
        P("seq", "head"),
        P("seq", "head"),
        P("head", "seq"),
        P("head"),
        P("seq", "head"),
    )
    out_specs = (P("seq", "head"), P("seq", "head"), P("seq", "head"), P("seq", "head"), P("head"))
    return jax.shard_map(
        functools.partial(on_device, mesh.shape["seq"], mesh.shape["head"]),
        mesh=mesh, in_specs=in_specs, out_specs=out_specs, check_vma=False,
    )
```
